256 devices in a mesh: dp: 128 (over y, z, x), head: 2 (over core).
Axes of the slice: x: 4, y: 4, z: 8, core: 2. Of those that a mesh axis runs over, the one named last changes fastest.
Arguments:
- teacher_hidden: bfloat16 [327680, 1024], P('dp', 'head'), may hold values from -6 to 6
- student_hidden: bfloat16 [327680, 312], P('dp'), may hold values from -6 to 6
- projector: bfloat16 [312, 1024], P(None, 'head'), may hold values from -0.3125 to 0.3125
- teacher_queries: bfloat16 [327680, 1024], P('dp', 'head'), may hold values from -6 to 6
- teacher_keys: bfloat16 [327680, 1024], P('dp', 'head'), may hold values from -6 to 6
- student_queries: bfloat16 [327680, 312], P('dp', 'head'), may hold values from -6 to 6
- student_keys: bfloat16 [327680, 312], P('dp', 'head'), may hold values from -6 to 6
- lengths: int32 [640], replicated, may hold values from 32 to 512, as said below
- plan: int32 [7, 128], replicated, may hold values from 0 to 4, as said below
Outputs:
- hidden_row: float32 [327680], P(('dp', 'head'))
- row_loss: float32 [128, 2, 5, 256], P('dp', 'head')
- loss: float32 [], replicated
The draws below stay inside these ranges and needn't reach their ends.
Inputs may be any that keep to these rules, and one draw needn't show every extreme that they name: lengths[k] counts the real tokens of the sequence in rows k * 512 onward, first held in slot k mod 5 of dp index k // 5; the rows after them are padding. Some sequence has exactly 512 tokens. In round r, dp index d gives the sequence in its slot plan[r, d] to dp index d XOR 2^r and receives that device's slot plan[r, d XOR 2^r] into the same slot; the rounds tend to even out the sum of squared lengths of the devices.
All inputs are finite; a program needn't handle non-finite values.
Results may differ from the reference program's by a relative error of at most 0.0003.
Values may be sent and summed in bfloat16 or wider, within the bound.
A program may use at most 128 MiB of HBM per device.

```python
import math
import jax
import jax.numpy as jnp
from jax import lax

HEADS_T = 16
HEAD_T = 64
HEADS_S = 12
HEAD_S = 26
MAXLEN = 512
SEQ_DEV = 5
D_T = 1024
D_S = 312
SEQS = 640
ROWS = 327680
ROUNDS = 7
N_HEAD = 2


def partner_rows_drawn(values, bit_index):
    block_span = 2 ** bit_index
    total_rows = values.shape[0]
    grouped = values.reshape((total_rows // (2 * block_span), 2, block_span) + values.shape[1:])
    return grouped[:, ::-1].reshape(values.shape)


def swap_slots_drawn(slot_table, chosen, bit_index):
    slot_order = jnp.arange(slot_table.shape[1], dtype=jnp.int32)
    partner_vals = partner_rows_drawn(slot_table, bit_index)
    partner_slot = partner_rows_drawn(chosen, bit_index)
    incoming = jnp.sum(jnp.where(slot_order[None, :] == partner_slot[:, None], partner_vals, 0), axis=1).astype(jnp.int32)
    return jnp.where(slot_order[None, :] == chosen[:, None], incoming[:, None], slot_table).astype(jnp.int32)


def shared_lengths(key):
    base_key = jax.random.fold_in(key, 7)
    shortest = MAXLEN // 16
    drawn_lengths = jax.random.randint(jax.random.fold_in(base_key, 1), (SEQS,), shortest, MAXLEN + 1, dtype=jnp.int32)
    marked = jax.random.permutation(jax.random.fold_in(base_key, 2), SEQS)
    positions = jnp.arange(SEQS, dtype=jnp.int32)
    drawn_lengths = jnp.where(positions == marked[0], MAXLEN, drawn_lengths)
    return jnp.where(positions == marked[1], shortest, drawn_lengths).astype(jnp.int32)


def draw_lengths(key, part):
    return shared_lengths(key)


def draw_plan(key, part):
    device_count = SEQS // SEQ_DEV
    slot_table = shared_lengths(key).reshape(device_count, SEQ_DEV)
    slot_order = jnp.arange(SEQ_DEV, dtype=jnp.int32)
    identity = jnp.arange(device_count, dtype=jnp.int32)
    chosen_rows = []
    for bit_index in range(ROUNDS):
        squares = slot_table * slot_table
        work_load = jnp.sum(squares, axis=1).astype(jnp.int32)
        partner_load = partner_rows_drawn(work_load, bit_index)
        partner_id = partner_rows_drawn(identity, bit_index)
        heavier = (work_load > partner_load) | (work_load == partner_load) & (identity > partner_id)
        longest = jnp.argmax(slot_table * SEQ_DEV + slot_order[None, :], axis=1).astype(jnp.int32)
        partner_big = partner_rows_drawn(jnp.max(squares, axis=1), bit_index)
        imbalance = jnp.abs(partner_load[:, None] - work_load[:, None] - 2 * partner_big[:, None] + 2 * squares)
        lightest = jnp.argmin(imbalance * SEQ_DEV + slot_order[None, :], axis=1).astype(jnp.int32)
        chosen = jnp.where(heavier, longest, lightest).astype(jnp.int32)
        chosen_rows.append(chosen)
        slot_table = swap_slots_drawn(slot_table, chosen, bit_index)
    return jnp.stack(chosen_rows).astype(jnp.int32)


def shard_levels(key, dims, split, low, high):
    def one(position, parts):
        steps = jax.random.uniform(jax.random.fold_in(jax.random.fold_in(key, 6), position), (parts,), jnp.float32, low / len(split), high / len(split))
        return jnp.repeat(jnp.exp(steps), dims[position] // parts).reshape((-1,) + (1,) * (len(dims) - position - 1))

    level = one(*split[0])
    for cut in split[1:]:
        level = level * one(*cut)
    return level


def scatter_about(own_key, dims, scale, reach, cuts=(), kind=jnp.bfloat16):
    entries = jax.random.normal(own_key, dims, jnp.float32) * scale
    if len(cuts) > 0:
        entries = shard_levels(own_key, dims, cuts, -0.22, 0.18) * entries
    return jnp.clip(entries, min=-reach, max=reach).astype(kind)


def setup_inputs(seed: int = 0) -> dict:
    key_list = jax.random.split(jax.random.key(seed), 10)
    teacher_hidden = scatter_about(key_list[0], (ROWS, D_T), 1.0, 6.0, ((0, 128), (1, 2)))
    student_hidden = scatter_about(key_list[1], (ROWS, D_S), 1.0, 6.0, ((0, 128),))
    projector = scatter_about(key_list[2], (D_S, D_T), D_S ** -0.5, 0.3125, ((1, 2),))
    teacher_queries = scatter_about(key_list[3], (ROWS, D_T), 1.0, 6.0, ((0, 128), (1, 2)))
    teacher_keys = scatter_about(key_list[4], (ROWS, D_T), 1.0, 6.0, ((0, 128), (1, 2)))
    student_queries = scatter_about(key_list[5], (ROWS, D_S), 1.0, 6.0, ((0, 128), (1, 2)))
    student_keys = scatter_about(key_list[6], (ROWS, D_S), 1.0, 6.0, ((0, 128), (1, 2)))
    lengths = draw_lengths(jax.random.fold_in(key_list[9], 71), 0)
    plan = draw_plan(jax.random.fold_in(key_list[9], 71), 0)
    return {"teacher_hidden": teacher_hidden, "student_hidden": student_hidden, "projector": projector, "teacher_queries": teacher_queries, "teacher_keys": teacher_keys, "student_queries": student_queries, "student_keys": student_keys, "lengths": lengths, "plan": plan}


def partner_rows(values, bit_index):
    block_span = 2 ** bit_index
    total_rows = values.shape[0]
    grouped = values.reshape((total_rows // (2 * block_span), 2, block_span) + values.shape[1:])
    return grouped[:, ::-1].reshape(values.shape)

def swap_slots(slot_table, chosen, bit_index):
    slot_order = jnp.arange(slot_table.shape[1], dtype=jnp.int32)
    partner_vals = partner_rows(slot_table, bit_index)
    partner_slot = partner_rows(chosen, bit_index)
    incoming = lax.optimization_barrier(jnp.sum(jnp.where(slot_order[None, :] == partner_slot[:, None], partner_vals, 0), axis=1)).astype(jnp.int32)
    return jnp.where(slot_order[None, :] == chosen[:, None], incoming[:, None], slot_table).astype(jnp.int32)

def reference(teacher_hidden, student_hidden, projector, teacher_queries, teacher_keys, student_queries, student_keys, lengths, plan):
    t_scale = 1.0 / (HEADS_T * math.sqrt(HEAD_T))
    s_scale = 1.0 / (HEADS_S * math.sqrt(HEAD_S))
    device_count = plan.shape[1]
    owner_table = jnp.arange(SEQS, dtype=jnp.int32).reshape(device_count, SEQ_DEV)
    for bit_index in range(plan.shape[0]):
        owner_table = swap_slots(owner_table, plan[bit_index].astype(jnp.int32), bit_index)
    positions = jnp.arange(MAXLEN, dtype=jnp.int32)

    def hidden_one(seq_index):
        row_start = (seq_index * MAXLEN).astype(jnp.int32)
        student = lax.dynamic_slice_in_dim(student_hidden, row_start, MAXLEN, 0)
        teacher = lax.dynamic_slice_in_dim(teacher_hidden, row_start, MAXLEN, 0).astype(jnp.float32)
        projected = jnp.dot(student, projector, preferred_element_type=jnp.float32)
        errors = lax.optimization_barrier(jnp.sum((projected - teacher) * (projected - teacher), axis=1)) / D_T
        return jnp.where(positions < lengths[seq_index], errors, 0.0)
    hidden_row = lax.map(hidden_one, jnp.arange(SEQS, dtype=jnp.int32)).reshape(ROWS)

    def attend_one(seq_index):
        row_start = (seq_index * MAXLEN).astype(jnp.int32)
        t_query = lax.dynamic_slice_in_dim(teacher_queries, row_start, MAXLEN, 0)
        t_key = lax.dynamic_slice_in_dim(teacher_keys, row_start, MAXLEN, 0)
        s_query = lax.dynamic_slice_in_dim(student_queries, row_start, MAXLEN, 0)
        s_key = lax.dynamic_slice_in_dim(student_keys, row_start, MAXLEN, 0)
        teacher_map = jnp.dot(t_query, t_key.T, preferred_element_type=jnp.float32)
        student_map = jnp.dot(s_query, s_key.T, preferred_element_type=jnp.float32)
        length = lengths[seq_index]
        inside = positions < length
        difference = jnp.where(inside[:, None] & inside[None, :], teacher_map * t_scale - student_map * s_scale, 0.0)
        squares = difference * difference
        return (lax.optimization_barrier(jnp.sum(squares, axis=1)) / length.astype(jnp.float32), jnp.sum(squares))
    per_row, seq_totals = lax.map(attend_one, owner_table.reshape(SEQS))
    row_loss = per_row.reshape(device_count, SEQ_DEV, N_HEAD, MAXLEN // N_HEAD).transpose(0, 2, 1, 3)
    lengths_float = lengths.astype(jnp.float32)
    loss = jnp.sum(hidden_row) / jnp.sum(lengths_float) + jnp.sum(seq_totals) / jnp.sum(lengths_float * lengths_float)
    return (hidden_row, row_loss, loss)
```

```python
import functools
import math

import jax
import jax.numpy as jnp
from jax import lax
from jax.experimental import pallas as pl
from jax.experimental.pallas import tpu as pltpu
from jax.sharding import Mesh
from jax.sharding import PartitionSpec as P

HEADS_T = 16
HEAD_T = 64
HEADS_S = 12
HEAD_S = 26
MAXLEN = 512
HALF = 256
SLOTS = 5
D_T = 1024
DP = ("dp_0", "dp_1", "dp_2")
DP_HEAD = ("dp_0", "dp_1", "dp_2", "head")
MESH = pl.DeviceIdType.MESH

T_SCALE = 1.0 / (HEADS_T * math.sqrt(HEAD_T))
S_SCALE = 1.0 / (HEADS_S * math.sqrt(HEAD_S))
KAPPA = S_SCALE / T_SCALE
OUT_SCALE = T_SCALE * T_SCALE


def flip(device, bit):
    mask = 2**bit
    return device + mask * (1 - 2 * ((device // mask) % 2))


def trace_forward(plan, device, slot, bits):
    for bit in bits:
        other = flip(device, bit)
        moves = plan[bit, device] == slot
        slot = jnp.where(moves, plan[bit, other], slot)
        device = jnp.where(moves, other, device)
    return device, slot


def trace_backward(plan, device, slot, bits):
    return trace_forward(plan, device, slot, tuple(reversed(bits)))


def kernel(
    sizes,
    bits,
    th,
    sht,
    pj,
    tq,
    tk,
    sqt,
    skt,
    lens,
    plan,
    hid_out,
    row_out,
    loss_out,
    tk_v,
    tq_v,
    sk_v,
    sq_v,
    th_v,
    sh_v,
    pj_v,
    len_v,
    len_s,
    plan_s,
    map_send,
    map_own,
    map_recv,
    hid_send,
    hid_recv,
    send_x,
    send_z,
    send_y,
    recv_x,
    recv_z,
    recv_y,
    cross_y,
    rows_x,
    rows_z,
    rows_y,
    load_sem,
    small_sem,
    map_ssem,
    map_rsem,
    hid_sem,
    ssem_x,
    rsem_x,
    ssem_z,
    rsem_z,
    ssem_y,
    rsem_y,
    ssem_c,
    rsem_c,
):
    ny, nz, nx = sizes
    y, z, x = (lax.axis_index(name) for name in DP)
    head = lax.axis_index("head")
    away = 1 - head
    me = (y * nz + z) * nx + x

    small = [
        pltpu.make_async_copy(plan, plan_s, small_sem.at[0]),
        pltpu.make_async_copy(lens, len_s, small_sem.at[1]),
        pltpu.make_async_copy(lens, len_v, small_sem.at[2]),
    ]
    loads = []
    for s in range(SLOTS):
        own = pl.multiple_of(s * MAXLEN + head * HALF, HALF)
        oth = pl.multiple_of(s * MAXLEN + away * HALF, HALF)
        n = 6 * s
        loads.append(
            [
                pltpu.make_async_copy(tk.at[pl.ds(s * MAXLEN, MAXLEN)], tk_v.at[s], load_sem.at[n]),
                pltpu.make_async_copy(tq.at[pl.ds(oth, HALF)], tq_v.at[s, 0], load_sem.at[n + 1]),
                pltpu.make_async_copy(
                    skt.at[:, pl.ds(s * MAXLEN, MAXLEN)], sk_v.at[s], load_sem.at[n + 2]
                ),
                pltpu.make_async_copy(sqt.at[:, pl.ds(oth, HALF)], sq_v.at[s, 0], load_sem.at[n + 3]),
                pltpu.make_async_copy(tq.at[pl.ds(own, HALF)], tq_v.at[s, 1], load_sem.at[n + 4]),
                pltpu.make_async_copy(sqt.at[:, pl.ds(own, HALF)], sq_v.at[s, 1], load_sem.at[n + 5]),
            ]
        )
    base = 6 * SLOTS
    load_pj = pltpu.make_async_copy(pj, pj_v, load_sem.at[base])
    hid_loads = []
    for b in range(2 * SLOTS):
        half = away if b < SLOTS else head
        first = pl.multiple_of((half * SLOTS + b % SLOTS) * HALF, HALF)
        n = base + 1 + 2 * b
        hid_loads.append(
            [
                pltpu.make_async_copy(sht.at[:, pl.ds(first, HALF)], sh_v.at[b], load_sem.at[n]),
                pltpu.make_async_copy(th.at[pl.ds(first, HALF)], th_v.at[b], load_sem.at[n + 1]),
            ]
        )
    for copy in loads[0]:
        copy.start()
    for copy in small:
        copy.start()
    for s in range(1, SLOTS):
        for copy in loads[s]:
            copy.start()
    load_pj.start()
    for pair in hid_loads:
        for copy in pair:
            copy.start()

    peers = [{"head": away}]
    peers += [{"dp_2": (x + k) % nx} for k in range(1, nx)]
    peers += [{"dp_1": (z + k) % nz} for k in range(1, nz)]
    peers += [{"dp_0": (y + k) % ny} for k in range(1, ny)]
    peers += [{"dp_0": (y + k) % ny, "head": away} for k in range(1, ny)]
    barrier = pltpu.get_barrier_semaphore()
    for peer in peers:
        pl.semaphore_signal(barrier, inc=1, device_id=peer, device_id_type=MESH)

    for copy in small:
        copy.wait()

    def length_of(slot):
        index = me * SLOTS + slot
        return len_s[index // 128, index % 128]

    coords = (x, z, y)
    strides = (1, nx, nx * nz)
    counts = (nx, nz, ny)
    gives, takes = [], []
    for coord, stride, count, rounds in zip(coords, strides, counts, bits):
        lands = [trace_forward(plan_s, me, s, rounds)[0] for s in range(SLOTS)]
        give = []
        for k in range(1, count):
            target = me + stride * ((coord + k) % count - coord)
            slot = jnp.int32(0)
            for s in range(SLOTS):
                slot = jnp.where(lands[s] == target, s, slot)
            give.append(slot)
        gives.append(give)
        take = []
        for s in range(SLOTS):
            device, slot = trace_backward(plan_s, me, s, rounds)
            source = (device // stride) % count
            take.append(jnp.where(device == me, 2 * count + slot, 2 * source))
        takes.append(take)

    def partial_map(s, half):
        teacher = lax.dot_general(
            tk_v[s], tq_v[s, half], (((1,), (1,)), ((), ())), preferred_element_type=jnp.float32
        )
        student = lax.dot_general(
            sk_v[s], sq_v[s, half], (((0,), (0,)), ((), ())), preferred_element_type=jnp.float32
        )
        return teacher - KAPPA * student

    map_copies = []
    for s in range(SLOTS):
        for copy in loads[s]:
            copy.wait()
        map_send[s] = partial_map(s, 0)
        if s == 0:
            pl.semaphore_wait(barrier, len(peers))
        copy = pltpu.make_async_remote_copy(
            src_ref=map_send.at[s],
            dst_ref=map_recv.at[s],
            send_sem=map_ssem.at[s],
            recv_sem=map_rsem.at[s],
            device_id={"head": away},
            device_id_type=MESH,
        )
        copy.start()
        map_copies.append(copy)
        map_own[s] = partial_map(s, 1)

    load_pj.wait()
    lane = lax.broadcasted_iota(jnp.int32, (1, HALF), 1)

    def hidden_block(b):
        for copy in hid_loads[b]:
            copy.wait()
        projected = lax.dot_general(
            sh_v[b], pj_v[...], (((0,), (0,)), ((), ())), preferred_element_type=jnp.float32
        )
        errors = projected - th_v[b].astype(jnp.float32)
        squares = errors * errors
        folded = squares[:, :128]
        for c in range(128, squares.shape[1], 128):
            folded = folded + squares[:, c : c + 128]
        sums = jnp.sum(folded.T, axis=0, keepdims=True)
        half = away if b < SLOTS else head
        block = half * SLOTS + b % SLOTS
        inside = lane + (block % 2) * HALF < length_of(block // 2)
        return jnp.where(inside, sums, 0.0)

    for b in range(SLOTS):
        hid_send[b] = hidden_block(b)
    hid_copy = pltpu.make_async_remote_copy(
        src_ref=hid_send,
        dst_ref=hid_recv,
        send_sem=hid_sem.at[0],
        recv_sem=hid_sem.at[1],
        device_id={"head": away},
        device_id_type=MESH,
    )
    hid_copy.start()
    own_hidden = [hidden_block(SLOTS + b) for b in range(SLOTS)]

    row_iota = lax.broadcasted_iota(jnp.int32, (8, HALF), 0)
    attention = jnp.zeros((1, HALF), jnp.float32)
    for s in range(SLOTS):
        map_copies[s].wait_recv()
        length = length_of(s)
        acc = jnp.zeros((8, HALF), jnp.float32)

        def chunk(c, acc, s=s, length=length):
            first = pl.multiple_of(c * 64, 64)
            whole = map_own[s, pl.ds(first, 64), :] + map_recv[s, pl.ds(first, 64), :]
            for r in range(8):
                part = whole[8 * r : 8 * r + 8, :]
                part = jnp.where(row_iota + (first + 8 * r) < length, part, 0.0)
                acc = acc + part * part
            return acc

        acc = lax.fori_loop(0, MAXLEN // 64, chunk, acc)
        sums = jnp.sum(acc, axis=0, keepdims=True) * OUT_SCALE
        sums = jnp.where(lane + head * HALF < length, sums, 0.0)
        attention = attention + sums
        rows_x[s] = sums / length.astype(jnp.float32)

    hid_copy.wait_recv()
    hidden = jnp.zeros((1, HALF), jnp.float32)
    for b in range(SLOTS):
        total = (own_hidden[b] + hid_recv[b]) * (1.0 / D_T)
        hid_out[2 * b : 2 * b + 1, :] = total[:, :128]
        hid_out[2 * b + 1 : 2 * b + 2, :] = total[:, 128:]
        hidden = hidden + total

    totals = jnp.concatenate(
        [hidden[:, :128] + hidden[:, 128:], attention[:, :128] + attention[:, 128:]], axis=1
    )

    def exchange(axis, coord, count, totals, rows, buffer, send, ssem, rsem, give):
        copies = []
        for k in range(1, count):
            send[2 * (k - 1)] = rows[give[k - 1]]
            send[2 * (k - 1) + 1] = totals
            copies.append(
                pltpu.make_async_remote_copy(
                    src_ref=send.at[pl.ds(2 * (k - 1), 2)],
                    dst_ref=buffer.at[pl.ds(2 * coord, 2)],
                    send_sem=ssem.at[k - 1],
                    recv_sem=rsem.at[k - 1],
                    device_id={axis: (coord + k) % count},
                    device_id_type=MESH,
                )
            )
            copies[-1].start()
        buffer[2 * coord + 1] = totals
        for s in range(SLOTS):
            buffer[2 * count + s] = rows[s]
        return copies

    def summed(rows):
        return functools.reduce(lambda a, b: a + b, rows)

    x_copies = exchange("dp_2", x, nx, totals, rows_x, recv_x, send_x, ssem_x, rsem_x, gives[0])
    for copy in x_copies:
        copy.wait_recv()
    for s in range(SLOTS):
        rows_z[s] = recv_x[takes[0][s]]
    totals = summed([recv_x[2 * i + 1] for i in range(nx)])

    z_copies = exchange("dp_1", z, nz, totals, rows_z, recv_z, send_z, ssem_z, rsem_z, gives[1])
    for copy in z_copies:
        copy.wait_recv()
    for s in range(SLOTS):
        rows_y[s] = recv_z[takes[1][s]]
    totals = summed([recv_z[2 * i + 1] for i in range(nz)])

    y_copies = exchange("dp_0", y, ny, totals, rows_y, recv_y, send_y, ssem_y, rsem_y, gives[2])
    crosses = []
    for k in range(ny):
        copy = pltpu.make_async_remote_copy(
            src_ref=send_y.at[pl.ds(1, 1)],
            dst_ref=cross_y.at[pl.ds(y, 1)],
            send_sem=ssem_c.at[k],
            recv_sem=rsem_c.at[k],
            device_id={"dp_0": (y + k) % ny, "head": away},
            device_id_type=MESH,
        )
        copy.start()
        crosses.append(copy)
    counted = len_v[...].astype(jnp.float32)
    tokens = jnp.sum(jnp.sum(counted, axis=0, keepdims=True), axis=1, keepdims=True)
    pairs = jnp.sum(jnp.sum(counted * counted, axis=0, keepdims=True), axis=1, keepdims=True)
    for copy in y_copies:
        copy.wait_recv()
    for s in range(SLOTS):
        row = recv_y[takes[2][s]]
        row_out[2 * s : 2 * s + 1, :] = row[:, :128]
        row_out[2 * s + 1 : 2 * s + 2, :] = row[:, 128:]
    for copy in crosses:
        copy.wait_recv()
    same = summed([recv_y[2 * i + 1] for i in range(ny)])
    cross = summed([cross_y[i] for i in range(ny)])
    totals = same + cross
    hidden_total = jnp.sum(totals[:, :128], axis=1, keepdims=True)
    attention_total = jnp.sum(totals[:, 128:], axis=1, keepdims=True)
    loss = hidden_total / tokens + attention_total / pairs
    loss_out[...] = jnp.broadcast_to(loss, loss_out.shape)

    for copy in map_copies + [hid_copy] + x_copies + z_copies + y_copies + crosses:
        copy.wait_send()


def body(sizes, bits, th, sh, pj, tq, tk, sq, sk, lengths, plan):
    ny, nz, nx = sizes
    rows = th.shape[0]
    d_s = sh.shape[1]
    half_t, half_s = tq.shape[1], sq.shape[1]
    bf16, f32 = jnp.bfloat16, jnp.float32
    table = lengths.reshape(-1, 128)
    any_spec = pl.BlockSpec(memory_space=pl.ANY)
    vmem_spec = pl.BlockSpec(memory_space=pltpu.VMEM)
    dma = pltpu.SemaphoreType.DMA
    scratch = [
        pltpu.VMEM((SLOTS, MAXLEN, half_t), bf16),
        pltpu.VMEM((SLOTS, 2, HALF, half_t), bf16),
        pltpu.VMEM((SLOTS, half_s, MAXLEN), bf16),
        pltpu.VMEM((SLOTS, 2, half_s, HALF), bf16),
        pltpu.VMEM((2 * SLOTS, HALF, half_t), bf16),
        pltpu.VMEM((2 * SLOTS, d_s, HALF), bf16),
        pltpu.VMEM((d_s, half_t), bf16),
        pltpu.VMEM(table.shape, jnp.int32),
        pltpu.SMEM(table.shape, jnp.int32),
        pltpu.SMEM(plan.shape, jnp.int32),
        pltpu.VMEM((SLOTS, MAXLEN, HALF), f32),
        pltpu.VMEM((SLOTS, MAXLEN, HALF), f32),
        pltpu.VMEM((SLOTS, MAXLEN, HALF), f32),
        pltpu.VMEM((SLOTS, 1, HALF), f32),
        pltpu.VMEM((SLOTS, 1, HALF), f32),
        pltpu.VMEM((2 * (nx - 1), 1, HALF), f32),
        pltpu.VMEM((2 * (nz - 1), 1, HALF), f32),
        pltpu.VMEM((2 * (ny - 1), 1, HALF), f32),
        pltpu.VMEM((2 * nx + SLOTS, 1, HALF), f32),
        pltpu.VMEM((2 * nz + SLOTS, 1, HALF), f32),
        pltpu.VMEM((2 * ny + SLOTS, 1, HALF), f32),
        pltpu.VMEM((ny, 1, HALF), f32),
        pltpu.VMEM((SLOTS, 1, HALF), f32),
        pltpu.VMEM((SLOTS, 1, HALF), f32),
        pltpu.VMEM((SLOTS, 1, HALF), f32),
        dma((6 * SLOTS + 1 + 4 * SLOTS,)),
        dma((3,)),
        dma((SLOTS,)),
        dma((SLOTS,)),
        dma((2,)),
        dma((nx - 1,)),
        dma((nx - 1,)),
        dma((nz - 1,)),
        dma((nz - 1,)),
        dma((ny - 1,)),
        dma((ny - 1,)),
        dma((ny,)),
        dma((ny,)),
    ]
    hid, row, loss = pl.pallas_call(
        functools.partial(kernel, sizes, bits),
        name="distill",
        out_shape=(
            jax.ShapeDtypeStruct((2 * SLOTS, 128), f32),
            jax.ShapeDtypeStruct((2 * SLOTS, 128), f32),
            jax.ShapeDtypeStruct((1, 128), f32),
        ),
        in_specs=[any_spec] * 9,
        out_specs=(vmem_spec,) * 3,
        scratch_shapes=scratch,
        compiler_params=pltpu.CompilerParams(
            collective_id=0, has_side_effects=True, vmem_limit_bytes=60 * 1024 * 1024
        ),
        cost_estimate=pl.CostEstimate(
            flops=3_500_000_000, bytes_accessed=12_000_000, transcendentals=0
        ),
    )(th, sh.T, pj, tq, tk, sq.T, sk.T, table, plan)
    return (
        hid.reshape(rows // 2),
        row.reshape(1, 1, SLOTS, HALF),
        loss[0, 0],
    )


def bit_groups(sizes):
    ny, nz, nx = sizes
    bx, bz, by = (n.bit_length() - 1 for n in (nx, nz, ny))
    return (
        tuple(range(bx)),
        tuple(range(bx, bx + bz)),
        tuple(range(bx + bz, bx + bz + by)),
    )


def solution(mesh, sizes=(4, 8, 4)):
    torus = Mesh(mesh.devices.reshape(*sizes, mesh.shape["head"]), DP_HEAD)
    placed = (
        P(DP, "head"),
        P(DP, None),
        P(None, "head"),
        P(DP, "head"),
        P(DP, "head"),
        P(DP, "head"),
        P(DP, "head"),
        P(),
        P(),
    )
    return jax.shard_map(
        functools.partial(body, sizes, bit_groups(sizes)),
        mesh=torus,
        in_specs=placed,
        out_specs=(P(DP_HEAD), P(DP, "head", None, None), P()),
        check_vma=False,
    )
```

```python
import functools
import math

import jax
import jax.numpy as jnp
from jax import lax
from jax.experimental import pallas as pl
from jax.experimental.pallas import tpu as pltpu
from jax.sharding import Mesh
from jax.sharding import PartitionSpec as P

HEADS_T = 16
HEAD_T = 64
HEADS_S = 12
HEAD_S = 26
MAXLEN = 512
HALF = 256
SLOTS = 5
D_T = 1024
DP = ("dp_0", "dp_1", "dp_2")
DP_HEAD = ("dp_0", "dp_1", "dp_2", "head")
MESH = pl.DeviceIdType.MESH

T_SCALE = 1.0 / (HEADS_T * math.sqrt(HEAD_T))
S_SCALE = 1.0 / (HEADS_S * math.sqrt(HEAD_S))
KAPPA = S_SCALE / T_SCALE
OUT_SCALE = T_SCALE * T_SCALE


def flip(device, bit):
    mask = 2**bit
    return device + mask * (1 - 2 * ((device // mask) % 2))


def trace_forward(plan, device, slot, bits):
    for bit in bits:
        other = flip(device, bit)
        moves = plan[bit, device] == slot
        slot = jnp.where(moves, plan[bit, other], slot)
        device = jnp.where(moves, other, device)
    return device, slot


def trace_backward(plan, device, slot, bits):
    return trace_forward(plan, device, slot, tuple(reversed(bits)))


def kernel(
    sizes,
    bits,
    th,
    sht,
    pj,
    tq,
    tk,
    sqt,
    skt,
    lens,
    plan,
    hid_out,
    row_out,
    loss_out,
    tk_v,
    tq_v,
    sk_v,
    sq_v,
    th_v,
    sh_v,
    pj_v,
    len_v,
    len_s,
    plan_s,
    map_send,
    map_own,
    map_recv,
    hid_send,
    hid_recv,
    send_a,
    send_b,
    recv_a,
    recv_b,
    cross_b,
    rows_a,
    rows_b,
    load_sem,
    small_sem,
    map_ssem,
    map_rsem,
    hid_sem,
    ssem_a,
    rsem_a,
    ssem_b,
    rsem_b,
    ssem_c,
    rsem_c,
):
    ny, nz, nx = sizes
    y, z, x = (lax.axis_index(name) for name in DP)
    head = lax.axis_index("head")
    away = 1 - head
    plane = nz * nx
    spot = z * nx + x
    me = y * plane + spot

    small = [
        pltpu.make_async_copy(plan, plan_s, small_sem.at[0]),
        pltpu.make_async_copy(lens, len_s, small_sem.at[1]),
        pltpu.make_async_copy(lens, len_v, small_sem.at[2]),
    ]
    loads = []
    for s in range(SLOTS):
        n = 6 * s
        copies = [
            pltpu.make_async_copy(tk.at[pl.ds(s * MAXLEN, MAXLEN)], tk_v.at[s], load_sem.at[n]),
            pltpu.make_async_copy(
                skt.at[:, pl.ds(s * MAXLEN, MAXLEN)], sk_v.at[s], load_sem.at[n + 1]
            ),
        ]
        for h, half in enumerate((away, head)):
            first = pl.multiple_of(s * MAXLEN + half * HALF, HALF)
            place = pl.ds(h * HALF, HALF)
            copies += [
                pltpu.make_async_copy(
                    tq.at[pl.ds(first, HALF)], tq_v.at[s, place], load_sem.at[n + 2 + 2 * h]
                ),
                pltpu.make_async_copy(
                    sqt.at[:, pl.ds(first, HALF)], sq_v.at[s, :, place], load_sem.at[n + 3 + 2 * h]
                ),
            ]
        loads.append(copies)
    base = 6 * SLOTS
    load_pj = pltpu.make_async_copy(pj, pj_v, load_sem.at[base])
    hid_loads = []
    for b in range(2 * SLOTS):
        half = away if b < SLOTS else head
        first = pl.multiple_of((half * SLOTS + b % SLOTS) * HALF, HALF)
        n = base + 1 + 2 * b
        hid_loads.append(
            [
                pltpu.make_async_copy(sht.at[:, pl.ds(first, HALF)], sh_v.at[b], load_sem.at[n]),
                pltpu.make_async_copy(th.at[pl.ds(first, HALF)], th_v.at[b], load_sem.at[n + 1]),
            ]
        )
    for copy in loads[0] + small:
        copy.start()

    offsets = [(dz, dx) for dz in range(nz) for dx in range(nx) if dz or dx]
    offsets.sort(key=lambda o: -min(o[0], nz - o[0]) - min(o[1], nx - o[1]))
    targets_a = [((z + dz) % nz, (x + dx) % nx) for dz, dx in offsets]
    peers = [{"head": away}]
    peers += [{"dp_1": tz, "dp_2": tx} for tz, tx in targets_a]
    peers += [{"dp_0": (y + k) % ny} for k in range(1, ny)]
    peers += [{"dp_0": (y + k) % ny, "head": away} for k in range(1, ny)]
    barrier = pltpu.get_barrier_semaphore()
    for copy in loads[1]:
        copy.start()
    for peer in peers:
        pl.semaphore_signal(barrier, inc=1, device_id=peer, device_id_type=MESH)
    for copy in loads[2]:
        copy.start()

    ahead = {0: loads[3], 1: loads[4], 2: [load_pj] + hid_loads[0] + hid_loads[1]}
    ahead[3] = hid_loads[2] + hid_loads[3] + hid_loads[4]
    ahead[4] = hid_loads[5] + hid_loads[6]
    later = {g: hid_loads[g + 7] for g in range(3)}

    def length_of(slot):
        index = me * SLOTS + slot
        return len_s[index // 128, index % 128]

    def routes():
        lands = [trace_forward(plan_s, me, s, bits[0])[0] for s in range(SLOTS)]
        gives_a = []
        for tz, tx in targets_a:
            target = y * plane + tz * nx + tx
            slot = jnp.int32(0)
            for s in range(1, SLOTS):
                slot = jnp.where(lands[s] == target, s, slot)
            gives_a.append(slot)
        lands = [trace_forward(plan_s, me, s, bits[1])[0] for s in range(SLOTS)]
        gives_b = []
        for k in range(1, ny):
            target = ((y + k) % ny) * plane + spot
            slot = jnp.int32(0)
            for s in range(1, SLOTS):
                slot = jnp.where(lands[s] == target, s, slot)
            gives_b.append(slot)
        takes = []
        for rounds, stride, count in ((bits[0], 1, plane), (bits[1], plane, ny)):
            take = []
            for s in range(SLOTS):
                device, slot = trace_backward(plan_s, me, s, rounds)
                source = (device // stride) % count
                take.append(jnp.where(device == me, 2 * count + slot, 2 * source))
            takes.append(take)
        return gives_a, gives_b, takes[0], takes[1]

    map_copies = []
    for s in range(SLOTS):
        for copy in loads[s]:
            copy.wait()
        if s == 0:
            for copy in small:
                copy.wait()
        for copy in ahead[s]:
            copy.start()
        teacher = lax.dot_general(
            tk_v[s], tq_v[s], (((1,), (1,)), ((), ())), preferred_element_type=jnp.float32
        )
        student = lax.dot_general(
            sk_v[s], sq_v[s], (((0,), (0,)), ((), ())), preferred_element_type=jnp.float32
        )
        partial = teacher - KAPPA * student
        map_send[s] = partial[:, :HALF]
        map_own[s] = partial[:, HALF:]
        if s == 0:
            gives_a, gives_b, takes_a, takes_b = routes()
            pl.semaphore_wait(barrier, len(peers))
        copy = pltpu.make_async_remote_copy(
            src_ref=map_send.at[s],
            dst_ref=map_recv.at[s],
            send_sem=map_ssem.at[s],
            recv_sem=map_rsem.at[s],
            device_id={"head": away},
            device_id_type=MESH,
        )
        copy.start()
        map_copies.append(copy)

    lane = lax.broadcasted_iota(jnp.int32, (1, HALF), 1)
    sublane = lax.broadcasted_iota(jnp.int32, (8, HALF), 0)

    def hidden_block(b):
        projected = lax.dot_general(
            sh_v[b], pj_v[...], (((0,), (0,)), ((), ())), preferred_element_type=jnp.float32
        )
        errors = projected - th_v[b].astype(jnp.float32)
        squares = errors * errors
        folded = squares[:, :128]
        for c in range(128, squares.shape[1], 128):
            folded = folded + squares[:, c : c + 128]
        sums = jnp.sum(folded.T, axis=0, keepdims=True)
        half = away if b < SLOTS else head
        block = half * SLOTS + b % SLOTS
        inside = lane + (block % 2) * HALF < length_of(block // 2)
        return jnp.where(inside, sums, 0.0)

    def row_sums(s):
        length = length_of(s)
        accs = [jnp.zeros((8, HALF), jnp.float32) for _ in range(4)]
        for r in range(MAXLEN // 8):
            part = map_own[s, 8 * r : 8 * r + 8, :] + map_recv[s, 8 * r : 8 * r + 8, :]
            part = jnp.where(sublane < length - 8 * r, part, 0.0)
            accs[r % 4] = accs[r % 4] + part * part
        acc = (accs[0] + accs[1]) + (accs[2] + accs[3])
        sums = jnp.sum(acc, axis=0, keepdims=True) * OUT_SCALE
        sums = jnp.where(lane + head * HALF < length, sums, 0.0)
        rows_a[s] = sums / length.astype(jnp.float32)
        return sums

    own_hidden = []
    attention = jnp.zeros((1, HALF), jnp.float32)
    load_pj.wait()
    for g in range(SLOTS):
        for b in (2 * g, 2 * g + 1):
            for copy in hid_loads[b]:
                copy.wait()
        for copy in later.get(g, ()):
            copy.start()
        map_copies[g].wait_recv()
        for b in (2 * g, 2 * g + 1):
            sums = hidden_block(b)
            if b < SLOTS:
                hid_send[b] = sums
            else:
                own_hidden.append(sums)
        attention = attention + row_sums(g)
        if 2 * g <= SLOTS - 1 <= 2 * g + 1:
            hid_copy = pltpu.make_async_remote_copy(
                src_ref=hid_send,
                dst_ref=hid_recv,
                send_sem=hid_sem.at[0],
                recv_sem=hid_sem.at[1],
                device_id={"head": away},
                device_id_type=MESH,
            )
            hid_copy.start()

    hid_copy.wait_recv()
    hidden = jnp.zeros((1, HALF), jnp.float32)
    for b in range(SLOTS):
        total = (own_hidden[b] + hid_recv[b]) * (1.0 / D_T)
        hid_out[2 * b : 2 * b + 1, :] = total[:, :128]
        hid_out[2 * b + 1 : 2 * b + 2, :] = total[:, 128:]
        hidden = hidden + total

    totals = jnp.concatenate(
        [hidden[:, :128] + hidden[:, 128:], attention[:, :128] + attention[:, 128:]], axis=1
    )

    def exchange(peers, slot, count, totals, rows, buffer, send, ssem, rsem, give):
        copies = []
        for k, peer in enumerate(peers):
            send[2 * k] = rows[give[k]]
            send[2 * k + 1] = totals
            copies.append(
                pltpu.make_async_remote_copy(
                    src_ref=send.at[pl.ds(2 * k, 2)],
                    dst_ref=buffer.at[pl.ds(2 * slot, 2)],
                    send_sem=ssem.at[k],
                    recv_sem=rsem.at[k],
                    device_id=peer,
                    device_id_type=MESH,
                )
            )
            copies[-1].start()
        buffer[2 * slot + 1] = totals
        for s in range(SLOTS):
            buffer[2 * count + s] = rows[s]
        return copies

    def summed(rows):
        while len(rows) > 1:
            rows = [functools.reduce(lambda a, b: a + b, rows[i : i + 2]) for i in range(0, len(rows), 2)]
        return rows[0]

    a_peers = [{"dp_1": tz, "dp_2": tx} for tz, tx in targets_a]
    a_copies = exchange(a_peers, spot, plane, totals, rows_a, recv_a, send_a, ssem_a, rsem_a, gives_a)
    counted = len_v[...].astype(jnp.float32)
    tokens = jnp.sum(jnp.sum(counted, axis=0, keepdims=True), axis=1, keepdims=True)
    pairs = jnp.sum(jnp.sum(counted * counted, axis=0, keepdims=True), axis=1, keepdims=True)
    for copy in a_copies:
        copy.wait_recv()
    for s in range(SLOTS):
        rows_b[s] = recv_a[takes_a[s]]
    totals = summed([recv_a[2 * i + 1] for i in range(plane)])

    b_peers = [{"dp_0": (y + k) % ny} for k in range(1, ny)]
    b_copies = exchange(b_peers, y, ny, totals, rows_b, recv_b, send_b, ssem_b, rsem_b, gives_b)
    crosses = []
    for k in range(ny):
        copy = pltpu.make_async_remote_copy(
            src_ref=send_b.at[pl.ds(1, 1)],
            dst_ref=cross_b.at[pl.ds(y, 1)],
            send_sem=ssem_c.at[k],
            recv_sem=rsem_c.at[k],
            device_id={"dp_0": (y + k) % ny, "head": away},
            device_id_type=MESH,
        )
        copy.start()
        crosses.append(copy)
    for copy in map_copies + [hid_copy] + a_copies:
        copy.wait_send()
    for copy in b_copies:
        copy.wait_recv()
    for s in range(SLOTS):
        row_out[s] = recv_b[takes_b[s]]
    for copy in crosses:
        copy.wait_recv()
    same = summed([recv_b[2 * i + 1] for i in range(ny)])
    cross = summed([cross_b[i] for i in range(ny)])
    totals = same + cross
    hidden_total = jnp.sum(totals[:, :128], axis=1, keepdims=True)
    attention_total = jnp.sum(totals[:, 128:], axis=1, keepdims=True)
    loss = hidden_total / tokens + attention_total / pairs
    loss_out[...] = jnp.broadcast_to(loss, loss_out.shape)

    for copy in b_copies + crosses:
        copy.wait_send()


def deliver(*refs):
    sources, targets, sem = refs[:3], refs[3:6], refs[6]
    copies = [
        pltpu.make_async_copy(source, target, sem.at[n])
        for n, (source, target) in enumerate(zip(sources, targets))
    ]
    for copy in copies:
        copy.start()
    for copy in copies:
        copy.wait()


def body(sizes, bits, th, sh, pj, tq, tk, sq, sk, lengths, plan):
    ny, nz, nx = sizes
    rows = th.shape[0]
    d_s = sh.shape[1]
    half_t, half_s = tq.shape[1], sq.shape[1]
    bf16, f32 = jnp.bfloat16, jnp.float32
    table = lengths.reshape(-1, 128)
    any_spec = pl.BlockSpec(memory_space=pl.ANY)
    vmem_spec = pl.BlockSpec(memory_space=pltpu.VMEM)
    dma = pltpu.SemaphoreType.DMA
    plane = nz * nx
    scratch = [
        pltpu.VMEM((SLOTS, MAXLEN, half_t), bf16),
        pltpu.VMEM((SLOTS, MAXLEN, half_t), bf16),
        pltpu.VMEM((SLOTS, half_s, MAXLEN), bf16),
        pltpu.VMEM((SLOTS, half_s, MAXLEN), bf16),
        pltpu.VMEM((2 * SLOTS, HALF, half_t), bf16),
        pltpu.VMEM((2 * SLOTS, d_s, HALF), bf16),
        pltpu.VMEM((d_s, half_t), bf16),
        pltpu.VMEM(table.shape, jnp.int32),
        pltpu.SMEM(table.shape, jnp.int32),
        pltpu.SMEM(plan.shape, jnp.int32),
        pltpu.VMEM((SLOTS, MAXLEN, HALF), f32),
        pltpu.VMEM((SLOTS, MAXLEN, HALF), f32),
        pltpu.VMEM((SLOTS, MAXLEN, HALF), f32),
        pltpu.VMEM((SLOTS, 1, HALF), f32),
        pltpu.VMEM((SLOTS, 1, HALF), f32),
        pltpu.VMEM((2 * (plane - 1), 1, HALF), f32),
        pltpu.VMEM((2 * (ny - 1), 1, HALF), f32),
        pltpu.VMEM((2 * plane + SLOTS, 1, HALF), f32),
        pltpu.VMEM((2 * ny + SLOTS, 1, HALF), f32),
        pltpu.VMEM((ny, 1, HALF), f32),
        pltpu.VMEM((SLOTS, 1, HALF), f32),
        pltpu.VMEM((SLOTS, 1, HALF), f32),
        dma((6 * SLOTS + 1 + 4 * SLOTS,)),
        dma((3,)),
        dma((SLOTS,)),
        dma((SLOTS,)),
        dma((2,)),
        dma((plane - 1,)),
        dma((plane - 1,)),
        dma((ny - 1,)),
        dma((ny - 1,)),
        dma((ny,)),
        dma((ny,)),
    ]
    shapes = ((2 * SLOTS, 128), (SLOTS, 1, HALF), (1, 128))
    results = pl.pallas_call(
        functools.partial(kernel, sizes, bits),
        name="distill",
        out_shape=tuple(pltpu.VMEM(shape, f32) for shape in shapes),
        in_specs=[any_spec] * 9,
        out_specs=(vmem_spec,) * 3,
        scratch_shapes=scratch,
        compiler_params=pltpu.CompilerParams(
            collective_id=0, has_side_effects=True, vmem_limit_bytes=60 * 1024 * 1024
        ),
        cost_estimate=pl.CostEstimate(
            flops=3_500_000_000, bytes_accessed=12_000_000, transcendentals=0
        ),
    )(th, sh.T, pj, tq, tk, sq.T, sk.T, table, plan)
    hid, row, loss = pl.pallas_call(
        deliver,
        name="deliver",
        out_shape=tuple(jax.ShapeDtypeStruct(shape, f32) for shape in shapes),
        in_specs=[vmem_spec] * 3,
        out_specs=(any_spec,) * 3,
        scratch_shapes=[dma((3,))],
    )(*(pltpu.with_memory_space_constraint(result, pltpu.VMEM) for result in results))
    return (
        hid.reshape(rows // 2),
        row.reshape(1, 1, SLOTS, HALF),
        loss[0, 0],
    )


def bit_groups(sizes):
    ny, nz, nx = sizes
    first = (nx * nz).bit_length() - 1
    return tuple(range(first)), tuple(range(first, first + ny.bit_length() - 1))


def solution(mesh, sizes=(4, 8, 4)):
    torus = Mesh(mesh.devices.reshape(*sizes, mesh.shape["head"]), DP_HEAD)
    placed = (
        P(DP, "head"),
        P(DP, None),
        P(None, "head"),
        P(DP, "head"),
        P(DP, "head"),
        P(DP, "head"),
        P(DP, "head"),
        P(),
        P(),
    )
    return jax.shard_map(
        functools.partial(body, sizes, bit_groups(sizes)),
        mesh=torus,
        in_specs=placed,
        out_specs=(P(DP_HEAD), P(DP, "head", None, None), P()),
        check_vma=False,
    )
```

```python
import functools
import math

import jax
import jax.numpy as jnp
from jax import lax
from jax.experimental import pallas as pl
from jax.experimental.pallas import tpu as pltpu
from jax.sharding import Mesh
from jax.sharding import PartitionSpec as P

HEADS_T = 16
HEAD_T = 64
HEADS_S = 12
HEAD_S = 26
MAXLEN = 512
HALF = 256
SLOTS = 5
D_T = 1024
DP = ("dp_0", "dp_1", "dp_2")
DP_HEAD = ("dp_0", "dp_1", "dp_2", "head")
MESH = pl.DeviceIdType.MESH

T_SCALE = 1.0 / (HEADS_T * math.sqrt(HEAD_T))
S_SCALE = 1.0 / (HEADS_S * math.sqrt(HEAD_S))
KAPPA = S_SCALE / T_SCALE
OUT_SCALE = T_SCALE * T_SCALE


def flip(device, bit):
    return lax.bitwise_xor(device, jnp.int32(2**bit))


def trace_forward(plan, device, slot, bits):
    for bit in bits:
        other = flip(device, bit)
        moves = plan[bit, device] == slot
        slot = jnp.where(moves, plan[bit, other], slot)
        device = jnp.where(moves, other, device)
    return device, slot


def trace_backward(plan, device, slot, bits):
    return trace_forward(plan, device, slot, tuple(reversed(bits)))


def kernel(
    sizes,
    bits,
    th,
    sht,
    pj,
    tq,
    tk,
    sqt,
    skt,
    lens,
    plan,
    hid_out,
    row_out,
    loss_out,
    tk_v,
    tq_v,
    sk_v,
    sq_v,
    th_v,
    sh_v,
    pj_v,
    len_v,
    len_s,
    plan_s,
    map_send,
    map_own,
    map_recv,
    hid_send,
    hid_recv,
    send_a,
    send_b,
    recv_a,
    recv_b,
    cross_b,
    rows_a,
    rows_b,
    load_sem,
    small_sem,
    map_ssem,
    map_rsem,
    hid_sem,
    ssem_a,
    rsem_a,
    ssem_b,
    rsem_b,
    ssem_c,
    rsem_c,
    greet_sem,
):
    ny, nz, nx = sizes
    y, z, x = (lax.axis_index(name) for name in DP)
    head = lax.axis_index("head")
    away = 1 - head
    plane = nz * nx
    spot = z * nx + x
    me = y * plane + spot

    small = [
        pltpu.make_async_copy(plan, plan_s, small_sem.at[0]),
        pltpu.make_async_copy(lens, len_s, small_sem.at[1]),
        pltpu.make_async_copy(lens, len_v, small_sem.at[2]),
    ]
    loads = []
    for s in range(SLOTS):
        n = 6 * s
        copies = [
            pltpu.make_async_copy(tk.at[pl.ds(s * MAXLEN, MAXLEN)], tk_v.at[s], load_sem.at[n]),
            pltpu.make_async_copy(
                skt.at[:, pl.ds(s * MAXLEN, MAXLEN)], sk_v.at[s], load_sem.at[n + 1]
            ),
        ]
        for h, half in enumerate((away, head)):
            first = pl.multiple_of(s * MAXLEN + half * HALF, HALF)
            place = pl.ds(h * HALF, HALF)
            copies += [
                pltpu.make_async_copy(
                    tq.at[pl.ds(first, HALF)], tq_v.at[s, place], load_sem.at[n + 2 + 2 * h]
                ),
                pltpu.make_async_copy(
                    sqt.at[:, pl.ds(first, HALF)], sq_v.at[s, :, place], load_sem.at[n + 3 + 2 * h]
                ),
            ]
        loads.append(copies)
    base = 6 * SLOTS
    load_pj = pltpu.make_async_copy(pj, pj_v, load_sem.at[base])
    hid_loads = []
    for b in range(2 * SLOTS):
        half = away if b < SLOTS else head
        first = pl.multiple_of((half * SLOTS + b % SLOTS) * HALF, HALF)
        n = base + 1 + 2 * b
        hid_loads.append(
            [
                pltpu.make_async_copy(sht.at[:, pl.ds(first, HALF)], sh_v.at[b], load_sem.at[n]),
                pltpu.make_async_copy(th.at[pl.ds(first, HALF)], th_v.at[b], load_sem.at[n + 1]),
            ]
        )
    for copy in small[:2] + loads[0] + small[2:]:
        copy.start()

    offsets = [(dz, dx) for dz in range(nz) for dx in range(nx) if dz or dx]
    offsets.sort(key=lambda o: -min(o[0], nz - o[0]) - min(o[1], nx - o[1]))
    targets_a = [((z + dz) % nz, (x + dx) % nx) for dz, dx in offsets]
    chips = [{"dp_1": tz, "dp_2": tx, "head": 1} for tz, tx in targets_a]
    chips += [{"dp_0": (y + k) % ny, "head": 1} for k in range(1, ny)]
    barrier = pltpu.get_barrier_semaphore()

    @pl.when(head == 1)
    def _():
        pl.semaphore_signal(barrier, inc=1, device_id={"head": 0}, device_id_type=MESH)

    for copy in loads[1]:
        copy.start()

    @pl.when(head == 0)
    def _():
        pl.semaphore_wait(barrier, 1)
        pl.semaphore_signal(greet_sem.at[0], inc=1, device_id={"head": 1}, device_id_type=MESH)

    @pl.when(head == 1)
    def _():
        pl.semaphore_wait(greet_sem.at[0], 1)
        for chip in chips:
            pl.semaphore_signal(barrier, inc=1, device_id=chip, device_id_type=MESH)

    for copy in loads[2]:
        copy.start()

    ahead = {0: loads[3], 1: loads[4], 2: [load_pj] + hid_loads[0] + hid_loads[1]}
    ahead[3] = hid_loads[2] + hid_loads[3] + hid_loads[4]
    ahead[4] = hid_loads[5] + hid_loads[6]
    later = {g: hid_loads[g + 7] for g in range(3)}

    def length_of(slot):
        index = me * SLOTS + slot
        return len_s[index // 128, index % 128]

    def routes():
        lands = [trace_forward(plan_s, me, s, bits[0])[0] for s in range(SLOTS)]
        gives_a = []
        for tz, tx in targets_a:
            target = y * plane + tz * nx + tx
            slot = jnp.int32(0)
            for s in range(1, SLOTS):
                slot = jnp.where(lands[s] == target, s, slot)
            gives_a.append(slot)
        lands = [trace_forward(plan_s, me, s, bits[1])[0] for s in range(SLOTS)]
        gives_b = []
        for k in range(1, ny):
            target = ((y + k) % ny) * plane + spot
            slot = jnp.int32(0)
            for s in range(1, SLOTS):
                slot = jnp.where(lands[s] == target, s, slot)
            gives_b.append(slot)
        takes = []
        for rounds, stride, count in ((bits[0], 1, plane), (bits[1], plane, ny)):
            take = []
            for s in range(SLOTS):
                device, slot = trace_backward(plan_s, me, s, rounds)
                source = lax.bitwise_and(
                    lax.shift_right_logical(device, jnp.int32(stride.bit_length() - 1)),
                    jnp.int32(count - 1),
                )
                take.append(jnp.where(device == me, 2 * count + slot, 2 * source))
            takes.append(take)
        return gives_a, gives_b, takes[0], takes[1]

    for copy in small:
        copy.wait()
    gives_a, gives_b, takes_a, takes_b = routes()
    map_copies = []
    for s in range(SLOTS):
        for copy in loads[s]:
            copy.wait()
        for copy in ahead[s]:
            copy.start()
        teacher = lax.dot_general(
            tk_v[s], tq_v[s], (((1,), (1,)), ((), ())), preferred_element_type=jnp.float32
        )
        student = lax.dot_general(
            sk_v[s], sq_v[s], (((0,), (0,)), ((), ())), preferred_element_type=jnp.float32
        )
        partial = teacher - KAPPA * student
        map_send[s] = partial[:, :HALF]
        map_own[s] = partial[:, HALF:]
        copy = pltpu.make_async_remote_copy(
            src_ref=map_send.at[s],
            dst_ref=map_recv.at[s],
            send_sem=map_ssem.at[s],
            recv_sem=map_rsem.at[s],
            device_id={"head": away},
            device_id_type=MESH,
        )
        copy.start()
        map_copies.append(copy)

    lane = lax.broadcasted_iota(jnp.int32, (1, HALF), 1)
    sublane = lax.broadcasted_iota(jnp.int32, (8, HALF), 0)

    def hidden_block(b):
        projected = lax.dot_general(
            sh_v[b], pj_v[...], (((0,), (0,)), ((), ())), preferred_element_type=jnp.float32
        )
        errors = projected - th_v[b].astype(jnp.float32)
        squares = errors * errors
        folded = squares[:, :128]
        for c in range(128, squares.shape[1], 128):
            folded = folded + squares[:, c : c + 128]
        sums = jnp.sum(folded.T, axis=0, keepdims=True)
        half = away if b < SLOTS else head
        block = half * SLOTS + b % SLOTS
        inside = lane + (block % 2) * HALF < length_of(block // 2)
        return jnp.where(inside, sums, 0.0)

    def row_sums(s):
        length = length_of(s)
        accs = [jnp.zeros((8, HALF), jnp.float32) for _ in range(4)]
        for r in range(MAXLEN // 8):
            part = map_own[s, 8 * r : 8 * r + 8, :] + map_recv[s, 8 * r : 8 * r + 8, :]
            part = jnp.where(sublane < length - 8 * r, part, 0.0)
            accs[r % 4] = accs[r % 4] + part * part
        acc = (accs[0] + accs[1]) + (accs[2] + accs[3])
        sums = jnp.sum(acc, axis=0, keepdims=True) * OUT_SCALE
        sums = jnp.where(lane + head * HALF < length, sums, 0.0)
        rows_a[s] = sums / length.astype(jnp.float32)
        return sums

    own_hidden = []
    attention = jnp.zeros((1, HALF), jnp.float32)
    load_pj.wait()
    for g in range(SLOTS):
        for b in (2 * g, 2 * g + 1):
            for copy in hid_loads[b]:
                copy.wait()
        for copy in later.get(g, ()):
            copy.start()
        map_copies[g].wait_recv()
        for b in (2 * g, 2 * g + 1):
            sums = hidden_block(b)
            if b < SLOTS:
                hid_send[b] = sums
            else:
                own_hidden.append(sums)
        attention = attention + row_sums(g)
        if 2 * g <= SLOTS - 1 <= 2 * g + 1:
            hid_copy = pltpu.make_async_remote_copy(
                src_ref=hid_send,
                dst_ref=hid_recv,
                send_sem=hid_sem.at[0],
                recv_sem=hid_sem.at[1],
                device_id={"head": away},
                device_id_type=MESH,
            )
            hid_copy.start()

    hid_copy.wait_recv()
    hidden = jnp.zeros((1, HALF), jnp.float32)
    for b in range(SLOTS):
        total = (own_hidden[b] + hid_recv[b]) * (1.0 / D_T)
        hid_out[2 * b : 2 * b + 1, :] = total[:, :128]
        hid_out[2 * b + 1 : 2 * b + 2, :] = total[:, 128:]
        hidden = hidden + total

    totals = jnp.concatenate(
        [hidden[:, :128] + hidden[:, 128:], attention[:, :128] + attention[:, 128:]], axis=1
    )

    def exchange(peers, slot, count, totals, rows, buffer, send, ssem, rsem, give):
        copies = []
        for k, peer in enumerate(peers):
            send[2 * k] = rows[give[k]]
            send[2 * k + 1] = totals
            copies.append(
                pltpu.make_async_remote_copy(
                    src_ref=send.at[pl.ds(2 * k, 2)],
                    dst_ref=buffer.at[pl.ds(2 * slot, 2)],
                    send_sem=ssem.at[k],
                    recv_sem=rsem.at[k],
                    device_id=peer,
                    device_id_type=MESH,
                )
            )
            copies[-1].start()
        buffer[2 * slot + 1] = totals
        for s in range(SLOTS):
            buffer[2 * count + s] = rows[s]
        return copies

    def summed(rows):
        while len(rows) > 1:
            rows = [functools.reduce(lambda a, b: a + b, rows[i : i + 2]) for i in range(0, len(rows), 2)]
        return rows[0]

    @pl.when(head == 1)
    def _():
        pl.semaphore_wait(barrier, len(chips))
        pl.semaphore_signal(greet_sem.at[1], inc=1, device_id={"head": 0}, device_id_type=MESH)

    @pl.when(head == 0)
    def _():
        pl.semaphore_wait(greet_sem.at[1], 1)

    a_peers = [{"dp_1": tz, "dp_2": tx} for tz, tx in targets_a]
    a_copies = exchange(a_peers, spot, plane, totals, rows_a, recv_a, send_a, ssem_a, rsem_a, gives_a)
    counted = len_v[...].astype(jnp.float32)
    tokens = jnp.sum(jnp.sum(counted, axis=0, keepdims=True), axis=1, keepdims=True)
    pairs = jnp.sum(jnp.sum(counted * counted, axis=0, keepdims=True), axis=1, keepdims=True)
    for copy in a_copies:
        copy.wait_recv()
    for s in range(SLOTS):
        rows_b[s] = recv_a[takes_a[s]]
    totals = summed([recv_a[2 * i + 1] for i in range(plane)])

    b_peers = [{"dp_0": (y + k) % ny} for k in range(1, ny)]
    b_copies = exchange(b_peers, y, ny, totals, rows_b, recv_b, send_b, ssem_b, rsem_b, gives_b)
    crosses = []
    for k in range(ny):
        copy = pltpu.make_async_remote_copy(
            src_ref=send_b.at[pl.ds(1, 1)],
            dst_ref=cross_b.at[pl.ds(y, 1)],
            send_sem=ssem_c.at[k],
            recv_sem=rsem_c.at[k],
            device_id={"dp_0": (y + k) % ny, "head": away},
            device_id_type=MESH,
        )
        copy.start()
        crosses.append(copy)
    for copy in map_copies + [hid_copy] + a_copies:
        copy.wait_send()
    for copy in b_copies:
        copy.wait_recv()
    for s in range(SLOTS):
        row_out[s] = recv_b[takes_b[s]]
    for copy in crosses:
        copy.wait_recv()
    same = summed([recv_b[2 * i + 1] for i in range(ny)])
    cross = summed([cross_b[i] for i in range(ny)])
    totals = same + cross
    hidden_total = jnp.sum(totals[:, :128], axis=1, keepdims=True)
    attention_total = jnp.sum(totals[:, 128:], axis=1, keepdims=True)
    loss = hidden_total / tokens + attention_total / pairs
    loss_out[...] = jnp.broadcast_to(loss, loss_out.shape)

    for copy in b_copies + crosses:
        copy.wait_send()


def deliver(*refs):
    sources, targets, sem = refs[:3], refs[3:6], refs[6]
    copies = [
        pltpu.make_async_copy(source, target, sem.at[n])
        for n, (source, target) in enumerate(zip(sources, targets))
    ]
    for copy in copies:
        copy.start()
    for copy in copies:
        copy.wait()


def body(sizes, bits, th, sh, pj, tq, tk, sq, sk, lengths, plan):
    ny, nz, nx = sizes
    rows = th.shape[0]
    d_s = sh.shape[1]
    half_t, half_s = tq.shape[1], sq.shape[1]
    bf16, f32 = jnp.bfloat16, jnp.float32
    table = lengths.reshape(-1, 128)
    any_spec = pl.BlockSpec(memory_space=pl.ANY)
    vmem_spec = pl.BlockSpec(memory_space=pltpu.VMEM)
    dma = pltpu.SemaphoreType.DMA
    plane = nz * nx
    scratch = [
        pltpu.VMEM((SLOTS, MAXLEN, half_t), bf16),
        pltpu.VMEM((SLOTS, MAXLEN, half_t), bf16),
        pltpu.VMEM((SLOTS, half_s, MAXLEN), bf16),
        pltpu.VMEM((SLOTS, half_s, MAXLEN), bf16),
        pltpu.VMEM((2 * SLOTS, HALF, half_t), bf16),
        pltpu.VMEM((2 * SLOTS, d_s, HALF), bf16),
        pltpu.VMEM((d_s, half_t), bf16),
        pltpu.VMEM(table.shape, jnp.int32),
        pltpu.SMEM(table.shape, jnp.int32),
        pltpu.SMEM(plan.shape, jnp.int32),
        pltpu.VMEM((SLOTS, MAXLEN, HALF), f32),
        pltpu.VMEM((SLOTS, MAXLEN, HALF), f32),
        pltpu.VMEM((SLOTS, MAXLEN, HALF), f32),
        pltpu.VMEM((SLOTS, 1, HALF), f32),
        pltpu.VMEM((SLOTS, 1, HALF), f32),
        pltpu.VMEM((2 * (plane - 1), 1, HALF), f32),
        pltpu.VMEM((2 * (ny - 1), 1, HALF), f32),
        pltpu.VMEM((2 * plane + SLOTS, 1, HALF), f32),
        pltpu.VMEM((2 * ny + SLOTS, 1, HALF), f32),
        pltpu.VMEM((ny, 1, HALF), f32),
        pltpu.VMEM((SLOTS, 1, HALF), f32),
        pltpu.VMEM((SLOTS, 1, HALF), f32),
        dma((6 * SLOTS + 1 + 4 * SLOTS,)),
        dma((3,)),
        dma((SLOTS,)),
        dma((SLOTS,)),
        dma((2,)),
        dma((plane - 1,)),
        dma((plane - 1,)),
        dma((ny - 1,)),
        dma((ny - 1,)),
        dma((ny,)),
        dma((ny,)),
        pltpu.SemaphoreType.REGULAR((2,)),
    ]
    shapes = ((2 * SLOTS, 128), (SLOTS, 1, HALF), (1, 128))
    results = pl.pallas_call(
        functools.partial(kernel, sizes, bits),
        name="distill",
        out_shape=tuple(pltpu.VMEM(shape, f32) for shape in shapes),
        in_specs=[any_spec] * 9,
        out_specs=(vmem_spec,) * 3,
        scratch_shapes=scratch,
        compiler_params=pltpu.CompilerParams(
            collective_id=0, has_side_effects=True, vmem_limit_bytes=60 * 1024 * 1024
        ),
        cost_estimate=pl.CostEstimate(
            flops=3_500_000_000, bytes_accessed=12_000_000, transcendentals=0
        ),
    )(th, sh.T, pj, tq, tk, sq.T, sk.T, table, plan)
    hid, row, loss = pl.pallas_call(
        deliver,
        name="deliver",
        out_shape=tuple(jax.ShapeDtypeStruct(shape, f32) for shape in shapes),
        in_specs=[vmem_spec] * 3,
        out_specs=(any_spec,) * 3,
        scratch_shapes=[dma((3,))],
    )(*(pltpu.with_memory_space_constraint(result, pltpu.VMEM) for result in results))
    return (
        hid.reshape(rows // 2),
        row.reshape(1, 1, SLOTS, HALF),
        loss[0, 0],
    )


def bit_groups(sizes):
    ny, nz, nx = sizes
    first = (nx * nz).bit_length() - 1
    return tuple(range(first)), tuple(range(first, first + ny.bit_length() - 1))


def solution(mesh, sizes=(4, 8, 4)):
    torus = Mesh(mesh.devices.reshape(*sizes, mesh.shape["head"]), DP_HEAD)
    placed = (
        P(DP, "head"),
        P(DP, None),
        P(None, "head"),
        P(DP, "head"),
        P(DP, "head"),
        P(DP, "head"),
        P(DP, "head"),
        P(),
        P(),
    )
    return jax.shard_map(
        functools.partial(body, sizes, bit_groups(sizes)),
        mesh=torus,
        in_specs=placed,
        out_specs=(P(DP_HEAD), P(DP, "head", None, None), P()),
        check_vma=False,
    )
```

```python
import functools
import math

import jax
import jax.numpy as jnp
from jax import lax
from jax.experimental import pallas as pl
from jax.experimental.pallas import tpu as pltpu
from jax.sharding import Mesh
from jax.sharding import PartitionSpec as P

HEADS_T = 16
HEAD_T = 64
HEADS_S = 12
HEAD_S = 26
MAXLEN = 512
HALF = 256
SLOTS = 5
D_T = 1024
DP = ("dp_0", "dp_1", "dp_2")
DP_HEAD = ("dp_0", "dp_1", "dp_2", "head")
MESH = pl.DeviceIdType.MESH

T_SCALE = 1.0 / (HEADS_T * math.sqrt(HEAD_T))
S_SCALE = 1.0 / (HEADS_S * math.sqrt(HEAD_S))
KAPPA = S_SCALE / T_SCALE
OUT_SCALE = T_SCALE * T_SCALE


def flip(device, bit):
    return lax.bitwise_xor(device, jnp.int32(2**bit))


def trace_forward(plan, device, slot, bits):
    for bit in bits:
        other = flip(device, bit)
        moves = plan[bit, device] == slot
        slot = jnp.where(moves, plan[bit, other], slot)
        device = jnp.where(moves, other, device)
    return device, slot


def trace_backward(plan, device, slot, bits):
    return trace_forward(plan, device, slot, tuple(reversed(bits)))


def kernel(
    sizes,
    bits,
    th,
    sht,
    pj,
    tq,
    tk,
    sqt,
    skt,
    lens,
    plan,
    hid_out,
    row_out,
    loss_out,
    tk_v,
    tq_v,
    sk_v,
    sq_v,
    th_v,
    sh_v,
    pj_v,
    len_v,
    len_s,
    plan_s,
    map_send,
    map_own,
    map_recv,
    hid_send,
    hid_recv,
    send_a,
    send_b,
    recv_a,
    recv_b,
    rows_a,
    rows_b,
    rows_c,
    load_sem,
    small_sem,
    map_ssem,
    map_rsem,
    hid_sem,
    ssem_a,
    rsem_a,
    ssem_b,
    rsem_b,
    own_sem,
    greet_sem,
):
    ny, nz, nx = sizes
    y, z, x = (lax.axis_index(name) for name in DP)
    head = lax.axis_index("head")
    away = 1 - head
    plane = nz * nx
    spot = z * nx + x
    me = y * plane + spot

    small = [
        pltpu.make_async_copy(plan, plan_s, small_sem.at[0]),
        pltpu.make_async_copy(lens, len_s, small_sem.at[1]),
        pltpu.make_async_copy(lens, len_v, small_sem.at[2]),
    ]
    loads = []
    for s in range(SLOTS):
        n = 6 * s
        copies = [
            pltpu.make_async_copy(tk.at[pl.ds(s * MAXLEN, MAXLEN)], tk_v.at[s], load_sem.at[n]),
            pltpu.make_async_copy(
                skt.at[:, pl.ds(s * MAXLEN, MAXLEN)], sk_v.at[s], load_sem.at[n + 1]
            ),
        ]
        for h, half in enumerate((away, head)):
            first = pl.multiple_of(s * MAXLEN + half * HALF, HALF)
            place = pl.ds(h * HALF, HALF)
            copies += [
                pltpu.make_async_copy(
                    tq.at[pl.ds(first, HALF)], tq_v.at[s, place], load_sem.at[n + 2 + 2 * h]
                ),
                pltpu.make_async_copy(
                    sqt.at[:, pl.ds(first, HALF)], sq_v.at[s, :, place], load_sem.at[n + 3 + 2 * h]
                ),
            ]
        loads.append(copies)
    base = 6 * SLOTS
    load_pj = pltpu.make_async_copy(pj, pj_v, load_sem.at[base])
    hid_loads = []
    for b in range(2 * SLOTS):
        half = away if b < SLOTS else head
        first = pl.multiple_of((half * SLOTS + b % SLOTS) * HALF, HALF)
        n = base + 1 + 2 * b
        hid_loads.append(
            [
                pltpu.make_async_copy(sht.at[:, pl.ds(first, HALF)], sh_v.at[b], load_sem.at[n]),
                pltpu.make_async_copy(th.at[pl.ds(first, HALF)], th_v.at[b], load_sem.at[n + 1]),
            ]
        )
    for copy in small[:2] + loads[0] + small[2:]:
        copy.start()

    offsets = [(dz, dx) for dz in range(nz) for dx in range(nx) if dz or dx]
    offsets.sort(key=lambda o: -min(o[0], nz - o[0]) - min(o[1], nx - o[1]))
    targets_a = [((z + dz) % nz, (x + dx) % nx) for dz, dx in offsets]
    chips = [{"dp_1": tz, "dp_2": tx, "head": 1} for tz, tx in targets_a]
    chips += [{"dp_0": (y + k) % ny, "head": 1} for k in range(1, ny)]
    barrier = pltpu.get_barrier_semaphore()

    @pl.when(head == 1)
    def _():
        pl.semaphore_signal(barrier, inc=1, device_id={"head": 0}, device_id_type=MESH)

    @pl.when(head == 0)
    def _():
        pl.semaphore_wait(barrier, 1)
        pl.semaphore_signal(greet_sem.at[0], inc=1, device_id={"head": 1}, device_id_type=MESH)

    @pl.when(head == 1)
    def _():
        pl.semaphore_wait(greet_sem.at[0], 1)
        for chip in chips:
            pl.semaphore_signal(barrier, inc=1, device_id=chip, device_id_type=MESH)

    def routes():
        lands = [trace_forward(plan_s, me, s, bits[0])[0] for s in range(SLOTS)]
        gives_a = []
        for tz, tx in targets_a:
            target = y * plane + tz * nx + tx
            slot = jnp.int32(0)
            for s in range(1, SLOTS):
                slot = jnp.where(lands[s] == target, s, slot)
            gives_a.append(slot)
        lands = [trace_forward(plan_s, me, s, bits[1])[0] for s in range(SLOTS)]
        gives_b = []
        for k in range(1, ny):
            target = ((y + k) % ny) * plane + spot
            slot = jnp.int32(0)
            for s in range(1, SLOTS):
                slot = jnp.where(lands[s] == target, s, slot)
            gives_b.append(slot)
        takes = []
        for rounds, stride, count in ((bits[0], 1, plane), (bits[1], plane, ny)):
            take = []
            for s in range(SLOTS):
                device, slot = trace_backward(plan_s, me, s, rounds)
                source = lax.bitwise_and(
                    lax.shift_right_logical(device, jnp.int32(stride.bit_length() - 1)),
                    jnp.int32(count - 1),
                )
                take.append(jnp.where(device == me, 2 * count + slot, 2 * source))
            takes.append(take)
        return gives_a, gives_b, takes[0], takes[1]

    for copy in loads[1]:
        copy.start()
    for copy in small:
        copy.wait()
    for copy in loads[2]:
        copy.start()
    gives_a, gives_b, takes_a, takes_b = routes()
    for copy in loads[3]:
        copy.start()

    ahead = {
        0: loads[4] + [load_pj] + hid_loads[0] + hid_loads[1],
        1: sum(hid_loads[2:6], []),
        3: sum(hid_loads[6:], []),
    }

    def length_of(slot):
        index = me * SLOTS + slot
        return len_s[index // 128, index % 128]

    map_copies = []
    for group in ((0,), (1, 2), (3, 4)):
        for s in group:
            for copy in loads[s]:
                copy.wait()
        for copy in ahead[group[0]]:
            copy.start()
        for s in group:
            teacher = lax.dot_general(
                tk_v[s], tq_v[s], (((1,), (1,)), ((), ())), preferred_element_type=jnp.float32
            )
            student = lax.dot_general(
                sk_v[s], sq_v[s], (((0,), (0,)), ((), ())), preferred_element_type=jnp.float32
            )
            partial = teacher - KAPPA * student
            map_send[s] = partial[:, :HALF]
            map_own[s] = partial[:, HALF:]
            copy = pltpu.make_async_remote_copy(
                src_ref=map_send.at[s],
                dst_ref=map_recv.at[s],
                send_sem=map_ssem.at[s],
                recv_sem=map_rsem.at[s],
                device_id={"head": away},
                device_id_type=MESH,
            )
            copy.start()
            map_copies.append(copy)

    lane = lax.broadcasted_iota(jnp.int32, (1, HALF), 1)
    sublane = lax.broadcasted_iota(jnp.int32, (8, HALF), 0)

    def hidden_block(b):
        projected = lax.dot_general(
            sh_v[b], pj_v[...], (((0,), (0,)), ((), ())), preferred_element_type=jnp.float32
        )
        errors = projected - th_v[b].astype(jnp.float32)
        squares = errors * errors
        folded = squares[:, :128]
        for c in range(128, squares.shape[1], 128):
            folded = folded + squares[:, c : c + 128]
        sums = jnp.sum(folded.T, axis=0, keepdims=True)
        half = away if b < SLOTS else head
        block = half * SLOTS + b % SLOTS
        inside = lane + (block % 2) * HALF < length_of(block // 2)
        return jnp.where(inside, sums, 0.0)

    def row_sums(s):
        length = length_of(s)
        accs = [jnp.zeros((8, HALF), jnp.float32) for _ in range(4)]
        for r in range(MAXLEN // 8):
            part = map_own[s, 8 * r : 8 * r + 8, :] + map_recv[s, 8 * r : 8 * r + 8, :]
            part = jnp.where(sublane < length - 8 * r, part, 0.0)
            accs[r % 4] = accs[r % 4] + part * part
        acc = (accs[0] + accs[1]) + (accs[2] + accs[3])
        sums = jnp.sum(acc, axis=0, keepdims=True) * OUT_SCALE
        sums = jnp.where(lane + head * HALF < length, sums, 0.0)
        rows_a[s] = sums / length.astype(jnp.float32)
        return sums

    hid_copy = pltpu.make_async_remote_copy(
        src_ref=hid_send,
        dst_ref=hid_recv,
        send_sem=hid_sem.at[0],
        recv_sem=hid_sem.at[1],
        device_id={"head": away},
        device_id_type=MESH,
    )
    attention = jnp.zeros((1, HALF), jnp.float32)
    load_pj.wait()
    for g in range(2):
        blocks = range(SLOTS * g, SLOTS * (g + 1))
        for b in blocks:
            for copy in hid_loads[b]:
                copy.wait()
        map_copies[g].wait_recv()
        own_hidden = [hidden_block(b) for b in blocks]
        attention = attention + row_sums(g)
        if g == 0:
            for b in blocks:
                hid_send[b] = own_hidden[b]
            hid_copy.start()
    for s in range(2, SLOTS):
        map_copies[s].wait_recv()
        attention = attention + row_sums(s)

    hid_copy.wait_recv()
    hidden = jnp.zeros((1, HALF), jnp.float32)
    for b in range(SLOTS):
        total = (own_hidden[b] + hid_recv[b]) * (1.0 / D_T)
        hid_out[2 * b : 2 * b + 1, :] = total[:, :128]
        hid_out[2 * b + 1 : 2 * b + 2, :] = total[:, 128:]
        hidden = hidden + total

    totals = jnp.concatenate(
        [hidden[:, :128] + hidden[:, 128:], attention[:, :128] + attention[:, 128:]], axis=1
    )

    @pl.when(head == 1)
    def _():
        pl.semaphore_wait(barrier, len(chips))
        pl.semaphore_signal(greet_sem.at[1], inc=1, device_id={"head": 0}, device_id_type=MESH)

    @pl.when(head == 0)
    def _():
        pl.semaphore_wait(greet_sem.at[1], 1)

    def summed(rows):
        while len(rows) > 1:
            rows = [
                functools.reduce(lambda a, b: a + b, rows[i : i + 2])
                for i in range(0, len(rows), 2)
            ]
        return rows[0]

    def first_copy(k, core):
        tz, tx = targets_a[k]
        return pltpu.make_async_remote_copy(
            src_ref=send_a.at[pl.ds(2 * k, 2)],
            dst_ref=recv_a.at[pl.ds(core * stretch + 2 * spot, 2)],
            send_sem=ssem_a.at[k],
            recv_sem=rsem_a.at[core * len(targets_a) + k],
            device_id={"dp_1": tz, "dp_2": tx, "head": 1},
            device_id_type=MESH,
        )

    stretch = 2 * plane + SLOTS + 1
    for k in range(len(targets_a)):
        send_a[2 * k] = rows_a[gives_a[k]]
        send_a[2 * k + 1] = totals
        first_copy(k, head).start()
    rows_a[SLOTS] = totals
    own_copy = pltpu.make_async_remote_copy(
        src_ref=rows_a,
        dst_ref=recv_a.at[pl.ds(2 * plane, SLOTS + 1)],
        send_sem=own_sem.at[0],
        recv_sem=own_sem.at[1],
        device_id={"head": 1},
        device_id_type=MESH,
    )

    @pl.when(head == 0)
    def _():
        own_copy.start()

    counted = len_v[...].astype(jnp.float32)
    tokens = jnp.sum(jnp.sum(counted, axis=0, keepdims=True), axis=1, keepdims=True)
    pairs = jnp.sum(jnp.sum(counted * counted, axis=0, keepdims=True), axis=1, keepdims=True)

    def second_copy(core, k):
        return pltpu.make_async_remote_copy(
            src_ref=send_b.at[pl.ds(2 * (core * (ny - 1) + k - 1), 2)],
            dst_ref=recv_b.at[pl.ds(2 * y, 2)],
            send_sem=ssem_b.at[core * (ny - 1) + k - 1],
            recv_sem=rsem_b.at[k - 1],
            device_id={"dp_0": (y + k) % ny, "head": core},
            device_id_type=MESH,
        )

    back_copy = pltpu.make_async_remote_copy(
        src_ref=rows_b,
        dst_ref=recv_b.at[pl.ds(2 * ny, SLOTS + 1)],
        send_sem=own_sem.at[2],
        recv_sem=own_sem.at[3],
        device_id={"head": 0},
        device_id_type=MESH,
    )

    @pl.when(head == 1)
    def _():
        for s in range(SLOTS + 1):
            recv_a[stretch + 2 * plane + s] = rows_a[s]
        own_copy.wait_recv()
        for core in range(2):
            recv_a[core * stretch + 2 * spot + 1] = recv_a[core * stretch + 2 * plane + SLOTS]
        for core in range(2):
            for k in range(len(targets_a)):
                first_copy(k, core).wait_recv()
        whole = summed(
            [recv_a[core * stretch + 2 * i + 1] for core in range(2) for i in range(plane)]
        )
        for s in range(SLOTS):
            rows_b[s] = recv_a[takes_a[s]]
            rows_c[s] = recv_a[stretch + takes_a[s]]
        for core in range(2):
            rows = (rows_b, rows_c)[core]
            for k in range(1, ny):
                place = 2 * (core * (ny - 1) + k - 1)
                send_b[place] = rows[gives_b[k - 1]]
                send_b[place + 1] = whole
                second_copy(core, k).start()
        rows_b[SLOTS] = whole
        back_copy.start()
        for s in range(SLOTS):
            recv_b[2 * ny + s] = rows_c[s]
        recv_b[2 * ny + SLOTS] = whole

    for copy in map_copies + [hid_copy]:
        copy.wait_send()
    for k in range(len(targets_a)):
        first_copy(k, head).wait_send()

    @pl.when(head == 0)
    def _():
        own_copy.wait_send()
        back_copy.wait_recv()

    recv_b[2 * y + 1] = recv_b[2 * ny + SLOTS]
    for k in range(1, ny):
        second_copy(0, k).wait_recv()
    for s in range(SLOTS):
        row_out[s] = recv_b[takes_b[s]]
    totals = summed([recv_b[2 * i + 1] for i in range(ny)])
    hidden_total = jnp.sum(totals[:, :128], axis=1, keepdims=True)
    attention_total = jnp.sum(totals[:, 128:], axis=1, keepdims=True)
    loss = hidden_total / tokens + attention_total / pairs
    loss_out[...] = jnp.broadcast_to(loss, loss_out.shape)

    @pl.when(head == 1)
    def _():
        for core in range(2):
            for k in range(1, ny):
                second_copy(core, k).wait_send()
        back_copy.wait_send()


def deliver(*refs):
    sources, targets, sem = refs[:3], refs[3:6], refs[6]
    copies = [
        pltpu.make_async_copy(source, target, sem.at[n])
        for n, (source, target) in enumerate(zip(sources, targets))
    ]
    for copy in copies:
        copy.start()
    for copy in copies:
        copy.wait()


def body(sizes, bits, th, sh, pj, tq, tk, sq, sk, lengths, plan):
    ny, nz, nx = sizes
    rows = th.shape[0]
    d_s = sh.shape[1]
    half_t, half_s = tq.shape[1], sq.shape[1]
    bf16, f32 = jnp.bfloat16, jnp.float32
    table = lengths.reshape(-1, 128)
    any_spec = pl.BlockSpec(memory_space=pl.ANY)
    vmem_spec = pl.BlockSpec(memory_space=pltpu.VMEM)
    dma = pltpu.SemaphoreType.DMA
    plane = nz * nx
    scratch = [
        pltpu.VMEM((SLOTS, MAXLEN, half_t), bf16),
        pltpu.VMEM((SLOTS, MAXLEN, half_t), bf16),
        pltpu.VMEM((SLOTS, half_s, MAXLEN), bf16),
        pltpu.VMEM((SLOTS, half_s, MAXLEN), bf16),
        pltpu.VMEM((2 * SLOTS, HALF, half_t), bf16),
        pltpu.VMEM((2 * SLOTS, d_s, HALF), bf16),
        pltpu.VMEM((d_s, half_t), bf16),
        pltpu.VMEM(table.shape, jnp.int32),
        pltpu.SMEM(table.shape, jnp.int32),
        pltpu.SMEM(plan.shape, jnp.int32),
        pltpu.VMEM((SLOTS, MAXLEN, HALF), f32),
        pltpu.VMEM((SLOTS, MAXLEN, HALF), f32),
        pltpu.VMEM((SLOTS, MAXLEN, HALF), f32),
        pltpu.VMEM((SLOTS, 1, HALF), f32),
        pltpu.VMEM((SLOTS, 1, HALF), f32),
        pltpu.VMEM((2 * (plane - 1), 1, HALF), f32),
        pltpu.VMEM((4 * (ny - 1), 1, HALF), f32),
        pltpu.VMEM((2 * (2 * plane + SLOTS + 1), 1, HALF), f32),
        pltpu.VMEM((2 * ny + SLOTS + 1, 1, HALF), f32),
        pltpu.VMEM((SLOTS + 1, 1, HALF), f32),
        pltpu.VMEM((SLOTS + 1, 1, HALF), f32),
        pltpu.VMEM((SLOTS, 1, HALF), f32),
        dma((6 * SLOTS + 1 + 4 * SLOTS,)),
        dma((3,)),
        dma((SLOTS,)),
        dma((SLOTS,)),
        dma((2,)),
        dma((plane - 1,)),
        dma((2 * (plane - 1),)),
        dma((2 * (ny - 1),)),
        dma((ny - 1,)),
        dma((4,)),
        pltpu.SemaphoreType.REGULAR((2,)),
    ]
    shapes = ((2 * SLOTS, 128), (SLOTS, 1, HALF), (1, 128))
    results = pl.pallas_call(
        functools.partial(kernel, sizes, bits),
        name="distill",
        out_shape=tuple(pltpu.VMEM(shape, f32) for shape in shapes),
        in_specs=[any_spec] * 9,
        out_specs=(vmem_spec,) * 3,
        scratch_shapes=scratch,
        compiler_params=pltpu.CompilerParams(
            collective_id=0, has_side_effects=True, vmem_limit_bytes=60 * 1024 * 1024
        ),
        cost_estimate=pl.CostEstimate(
            flops=3_500_000_000, bytes_accessed=12_000_000, transcendentals=0
        ),
    )(th, sh.T, pj, tq, tk, sq.T, sk.T, table, plan)
    hid, row, loss = pl.pallas_call(
        deliver,
        name="deliver",
        out_shape=tuple(jax.ShapeDtypeStruct(shape, f32) for shape in shapes),
        in_specs=[vmem_spec] * 3,
        out_specs=(any_spec,) * 3,
        scratch_shapes=[dma((3,))],
    )(*(pltpu.with_memory_space_constraint(result, pltpu.VMEM) for result in results))
    return (
        hid.reshape(rows // 2),
        row.reshape(1, 1, SLOTS, HALF),
        loss[0, 0],
    )


def bit_groups(sizes):
    ny, nz, nx = sizes
    first = (nx * nz).bit_length() - 1
    return tuple(range(first)), tuple(range(first, first + ny.bit_length() - 1))


def solution(mesh, sizes=(4, 8, 4)):
    torus = Mesh(mesh.devices.reshape(*sizes, mesh.shape["head"]), DP_HEAD)
    placed = (
        P(DP, "head"),
        P(DP, None),
        P(None, "head"),
        P(DP, "head"),
        P(DP, "head"),
        P(DP, "head"),
        P(DP, "head"),
        P(),
        P(),
    )
    return jax.shard_map(
        functools.partial(body, sizes, bit_groups(sizes)),
        mesh=torus,
        in_specs=placed,
        out_specs=(P(DP_HEAD), P(DP, "head", None, None), P()),
        check_vma=False,
    )
```

```python
import functools
import math

import jax
import jax.numpy as jnp
from jax import lax
from jax.experimental import pallas as pl
from jax.experimental.pallas import tpu as pltpu
from jax.sharding import Mesh
from jax.sharding import PartitionSpec as P

HEADS_T = 16
HEAD_T = 64
HEADS_S = 12
HEAD_S = 26
MAXLEN = 512
HALF = 256
SLOTS = 5
D_T = 1024
DP = ("dp_0", "dp_1", "dp_2")
DP_HEAD = ("dp_0", "dp_1", "dp_2", "head")
MESH = pl.DeviceIdType.MESH

T_SCALE = 1.0 / (HEADS_T * math.sqrt(HEAD_T))
S_SCALE = 1.0 / (HEADS_S * math.sqrt(HEAD_S))
KAPPA = S_SCALE / T_SCALE
OUT_SCALE = T_SCALE * T_SCALE


def flip(device, bit):
    return lax.bitwise_xor(device, jnp.int32(2**bit))


def trace_forward(plan, device, slot, bits):
    for bit in bits:
        other = flip(device, bit)
        moves = plan[bit, device] == slot
        slot = jnp.where(moves, plan[bit, other], slot)
        device = jnp.where(moves, other, device)
    return device, slot


def trace_backward(plan, device, slot, bits):
    return trace_forward(plan, device, slot, tuple(reversed(bits)))


def kernel(
    sizes,
    bits,
    th,
    sht,
    pj,
    tq,
    tk,
    sqt,
    skt,
    lens,
    plan,
    hid_out,
    row_out,
    loss_out,
    tk_v,
    tq_v,
    sk_v,
    sq_v,
    th_v,
    sh_v,
    pj_v,
    len_v,
    len_s,
    plan_s,
    map_send,
    map_own,
    map_recv,
    hid_send,
    hid_recv,
    send_a,
    send_b,
    recv_a,
    recv_b,
    rows_a,
    rows_b,
    rows_c,
    load_sem,
    small_sem,
    map_ssem,
    map_rsem,
    hid_sem,
    ssem_a,
    rsem_a,
    ssem_b,
    rsem_b,
    own_sem,
    greet_sem,
):
    ny, nz, nx = sizes
    y, z, x = (lax.axis_index(name) for name in DP)
    head = lax.axis_index("head")
    away = 1 - head
    plane = nz * nx
    spot = z * nx + x
    me = y * plane + spot

    small = [
        pltpu.make_async_copy(plan, plan_s, small_sem.at[0]),
        pltpu.make_async_copy(lens, len_s, small_sem.at[1]),
        pltpu.make_async_copy(lens, len_v, small_sem.at[2]),
    ]
    loads = []
    for s in range(SLOTS):
        n = 6 * s
        copies = [
            pltpu.make_async_copy(tk.at[pl.ds(s * MAXLEN, MAXLEN)], tk_v.at[s], load_sem.at[n]),
            pltpu.make_async_copy(
                skt.at[:, pl.ds(s * MAXLEN, MAXLEN)], sk_v.at[s], load_sem.at[n + 1]
            ),
        ]
        for h, half in enumerate((away, head)):
            first = pl.multiple_of(s * MAXLEN + half * HALF, HALF)
            place = pl.ds(h * HALF, HALF)
            copies += [
                pltpu.make_async_copy(
                    tq.at[pl.ds(first, HALF)], tq_v.at[s, place], load_sem.at[n + 2 + 2 * h]
                ),
                pltpu.make_async_copy(
                    sqt.at[:, pl.ds(first, HALF)], sq_v.at[s, :, place], load_sem.at[n + 3 + 2 * h]
                ),
            ]
        loads.append(copies)
    base = 6 * SLOTS
    load_pj = pltpu.make_async_copy(pj, pj_v, load_sem.at[base])
    hid_loads = []
    for b in range(2 * SLOTS):
        half = away if b < SLOTS else head
        first = pl.multiple_of((half * SLOTS + b % SLOTS) * HALF, HALF)
        n = base + 1 + 2 * b
        hid_loads.append(
            [
                pltpu.make_async_copy(sht.at[:, pl.ds(first, HALF)], sh_v.at[b], load_sem.at[n]),
                pltpu.make_async_copy(th.at[pl.ds(first, HALF)], th_v.at[b], load_sem.at[n + 1]),
            ]
        )
    for copy in small[:2] + loads[0] + small[2:]:
        copy.start()

    offsets = [(dz, dx) for dz in range(nz) for dx in range(nx) if dz or dx]
    offsets.sort(key=lambda o: -min(o[0], nz - o[0]) - min(o[1], nx - o[1]))
    targets_a = [((z + dz) % nz, (x + dx) % nx) for dz, dx in offsets]
    chips = [{"dp_1": tz, "dp_2": tx, "head": 1} for tz, tx in targets_a]
    chips += [{"dp_0": (y + k) % ny, "head": 1} for k in range(1, ny)]
    barrier = pltpu.get_barrier_semaphore()

    @pl.when(head == 1)
    def _():
        pl.semaphore_signal(barrier, inc=1, device_id={"head": 0}, device_id_type=MESH)

    @pl.when(head == 0)
    def _():
        pl.semaphore_wait(barrier, 1)
        pl.semaphore_signal(greet_sem.at[0], inc=1, device_id={"head": 1}, device_id_type=MESH)

    @pl.when(head == 1)
    def _():
        pl.semaphore_wait(greet_sem.at[0], 1)
        for chip in chips:
            pl.semaphore_signal(barrier, inc=1, device_id=chip, device_id_type=MESH)

    def routes():
        lands = [trace_forward(plan_s, me, s, bits[0])[0] for s in range(SLOTS)]
        gives_a = []
        for tz, tx in targets_a:
            target = y * plane + tz * nx + tx
            slot = jnp.int32(0)
            for s in range(1, SLOTS):
                slot = jnp.where(lands[s] == target, s, slot)
            gives_a.append(slot)
        lands = [trace_forward(plan_s, me, s, bits[1])[0] for s in range(SLOTS)]
        gives_b = []
        for k in range(1, ny):
            target = ((y + k) % ny) * plane + spot
            slot = jnp.int32(0)
            for s in range(1, SLOTS):
                slot = jnp.where(lands[s] == target, s, slot)
            gives_b.append(slot)
        takes = []
        for rounds, stride, count in ((bits[0], 1, plane), (bits[1], plane, ny)):
            take = []
            for s in range(SLOTS):
                device, slot = trace_backward(plan_s, me, s, rounds)
                source = lax.bitwise_and(
                    lax.shift_right_logical(device, jnp.int32(stride.bit_length() - 1)),
                    jnp.int32(count - 1),
                )
                take.append(jnp.where(device == me, 2 * count + slot, 2 * source))
            takes.append(take)
        return gives_a, gives_b, takes[0], takes[1]

    for copy in loads[1]:
        copy.start()
    for copy in loads[2] + loads[3]:
        copy.start()

    ahead = {
        0: loads[4] + [load_pj] + hid_loads[0] + hid_loads[1],
        1: sum(hid_loads[2:6], []),
        3: sum(hid_loads[6:], []),
    }

    def length_of(slot):
        index = me * SLOTS + slot
        return len_s[index // 128, index % 128]

    map_copies = []
    for group in ((0,), (1, 2), (3, 4)):
        for s in group:
            for copy in loads[s]:
                copy.wait()
        for copy in ahead[group[0]]:
            copy.start()
        for s in group:
            teacher = lax.dot_general(
                tk_v[s], tq_v[s], (((1,), (1,)), ((), ())), preferred_element_type=jnp.float32
            )
            student = lax.dot_general(
                sk_v[s], sq_v[s], (((0,), (0,)), ((), ())), preferred_element_type=jnp.float32
            )
            partial = teacher - KAPPA * student
            map_send[s] = partial[:, :HALF]
            map_own[s] = partial[:, HALF:]
            copy = pltpu.make_async_remote_copy(
                src_ref=map_send.at[s],
                dst_ref=map_recv.at[s],
                send_sem=map_ssem.at[s],
                recv_sem=map_rsem.at[s],
                device_id={"head": away},
                device_id_type=MESH,
            )
            copy.start()
            map_copies.append(copy)
        if group == (0,):
            for copy in small:
                copy.wait()
            gives_a, gives_b, takes_a, takes_b = routes()

    lane = lax.broadcasted_iota(jnp.int32, (1, HALF), 1)
    sublane = lax.broadcasted_iota(jnp.int32, (8, HALF), 0)

    def hidden_block(b):
        projected = lax.dot_general(
            sh_v[b], pj_v[...], (((0,), (0,)), ((), ())), preferred_element_type=jnp.float32
        )
        errors = projected - th_v[b].astype(jnp.float32)
        squares = errors * errors
        folded = squares[:, :128]
        for c in range(128, squares.shape[1], 128):
            folded = folded + squares[:, c : c + 128]
        sums = jnp.sum(folded.T, axis=0, keepdims=True)
        half = away if b < SLOTS else head
        block = half * SLOTS + b % SLOTS
        inside = lane + (block % 2) * HALF < length_of(block // 2)
        return jnp.where(inside, sums, 0.0)

    def row_sums(s):
        length = length_of(s)
        accs = [jnp.zeros((8, HALF), jnp.float32) for _ in range(4)]
        for r in range(MAXLEN // 8):
            part = map_own[s, 8 * r : 8 * r + 8, :] + map_recv[s, 8 * r : 8 * r + 8, :]
            part = jnp.where(sublane < length - 8 * r, part, 0.0)
            accs[r % 4] = accs[r % 4] + part * part
        acc = (accs[0] + accs[1]) + (accs[2] + accs[3])
        sums = jnp.sum(acc, axis=0, keepdims=True) * OUT_SCALE
        sums = jnp.where(lane + head * HALF < length, sums, 0.0)
        rows_a[s] = sums / length.astype(jnp.float32)
        return sums

    hid_copy = pltpu.make_async_remote_copy(
        src_ref=hid_send,
        dst_ref=hid_recv,
        send_sem=hid_sem.at[0],
        recv_sem=hid_sem.at[1],
        device_id={"head": away},
        device_id_type=MESH,
    )
    attention = jnp.zeros((1, HALF), jnp.float32)
    load_pj.wait()
    for g in range(2):
        blocks = range(SLOTS * g, SLOTS * (g + 1))
        for b in blocks:
            for copy in hid_loads[b]:
                copy.wait()
        map_copies[g].wait_recv()
        own_hidden = [hidden_block(b) for b in blocks]
        attention = attention + row_sums(g)
        if g == 0:
            for b in blocks:
                hid_send[b] = own_hidden[b]
            hid_copy.start()
    for s in range(2, SLOTS):
        map_copies[s].wait_recv()
        attention = attention + row_sums(s)

    hid_copy.wait_recv()
    hidden = jnp.zeros((1, HALF), jnp.float32)
    for b in range(SLOTS):
        total = (own_hidden[b] + hid_recv[b]) * (1.0 / D_T)
        hid_out[2 * b : 2 * b + 1, :] = total[:, :128]
        hid_out[2 * b + 1 : 2 * b + 2, :] = total[:, 128:]
        hidden = hidden + total

    totals = jnp.concatenate(
        [hidden[:, :128] + hidden[:, 128:], attention[:, :128] + attention[:, 128:]], axis=1
    )

    @pl.when(head == 1)
    def _():
        pl.semaphore_wait(barrier, len(chips))
        pl.semaphore_signal(greet_sem.at[1], inc=1, device_id={"head": 0}, device_id_type=MESH)

    @pl.when(head == 0)
    def _():
        pl.semaphore_wait(greet_sem.at[1], 1)

    def summed(rows):
        while len(rows) > 1:
            rows = [
                functools.reduce(lambda a, b: a + b, rows[i : i + 2])
                for i in range(0, len(rows), 2)
            ]
        return rows[0]

    def first_copy(k, core):
        tz, tx = targets_a[k]
        return pltpu.make_async_remote_copy(
            src_ref=send_a.at[pl.ds(2 * k, 2)],
            dst_ref=recv_a.at[pl.ds(core * stretch + 2 * spot, 2)],
            send_sem=ssem_a.at[k],
            recv_sem=rsem_a.at[core * len(targets_a) + k],
            device_id={"dp_1": tz, "dp_2": tx, "head": 1},
            device_id_type=MESH,
        )

    stretch = 2 * plane + SLOTS + 1
    for k in range(len(targets_a)):
        send_a[2 * k] = rows_a[gives_a[k]]
        send_a[2 * k + 1] = totals
        first_copy(k, head).start()
    rows_a[SLOTS] = totals
    own_copy = pltpu.make_async_remote_copy(
        src_ref=rows_a,
        dst_ref=recv_a.at[pl.ds(2 * plane, SLOTS + 1)],
        send_sem=own_sem.at[0],
        recv_sem=own_sem.at[1],
        device_id={"head": 1},
        device_id_type=MESH,
    )

    @pl.when(head == 0)
    def _():
        own_copy.start()

    counted = len_v[...].astype(jnp.float32)
    tokens = jnp.sum(jnp.sum(counted, axis=0, keepdims=True), axis=1, keepdims=True)
    pairs = jnp.sum(jnp.sum(counted * counted, axis=0, keepdims=True), axis=1, keepdims=True)

    def second_copy(core, k):
        return pltpu.make_async_remote_copy(
            src_ref=send_b.at[pl.ds(2 * (core * (ny - 1) + k - 1), 2)],
            dst_ref=recv_b.at[pl.ds(2 * y, 2)],
            send_sem=ssem_b.at[core * (ny - 1) + k - 1],
            recv_sem=rsem_b.at[k - 1],
            device_id={"dp_0": (y + k) % ny, "head": core},
            device_id_type=MESH,
        )

    back_copy = pltpu.make_async_remote_copy(
        src_ref=rows_b,
        dst_ref=recv_b.at[pl.ds(2 * ny, SLOTS + 1)],
        send_sem=own_sem.at[2],
        recv_sem=own_sem.at[3],
        device_id={"head": 0},
        device_id_type=MESH,
    )

    @pl.when(head == 1)
    def _():
        for s in range(SLOTS + 1):
            recv_a[stretch + 2 * plane + s] = rows_a[s]
        own_copy.wait_recv()
        for core in range(2):
            recv_a[core * stretch + 2 * spot + 1] = recv_a[core * stretch + 2 * plane + SLOTS]
        for core in range(2):
            for k in range(len(targets_a)):
                first_copy(k, core).wait_recv()
        whole = summed(
            [recv_a[core * stretch + 2 * i + 1] for core in range(2) for i in range(plane)]
        )
        for s in range(SLOTS):
            rows_b[s] = recv_a[takes_a[s]]
            rows_c[s] = recv_a[stretch + takes_a[s]]
        for core in range(2):
            rows = (rows_b, rows_c)[core]
            for k in range(1, ny):
                place = 2 * (core * (ny - 1) + k - 1)
                send_b[place] = rows[gives_b[k - 1]]
                send_b[place + 1] = whole
                second_copy(core, k).start()
        rows_b[SLOTS] = whole
        back_copy.start()
        for s in range(SLOTS):
            recv_b[2 * ny + s] = rows_c[s]
        recv_b[2 * ny + SLOTS] = whole

    for copy in map_copies + [hid_copy]:
        copy.wait_send()
    for k in range(len(targets_a)):
        first_copy(k, head).wait_send()

    @pl.when(head == 0)
    def _():
        own_copy.wait_send()
        back_copy.wait_recv()

    recv_b[2 * y + 1] = recv_b[2 * ny + SLOTS]
    for k in range(1, ny):
        second_copy(0, k).wait_recv()
    for s in range(SLOTS):
        row_out[s] = recv_b[takes_b[s]]
    totals = summed([recv_b[2 * i + 1] for i in range(ny)])
    hidden_total = jnp.sum(totals[:, :128], axis=1, keepdims=True)
    attention_total = jnp.sum(totals[:, 128:], axis=1, keepdims=True)
    loss = hidden_total / tokens + attention_total / pairs
    loss_out[...] = jnp.broadcast_to(loss, loss_out.shape)

    @pl.when(head == 1)
    def _():
        for core in range(2):
            for k in range(1, ny):
                second_copy(core, k).wait_send()
        back_copy.wait_send()


def deliver(*refs):
    sources, targets, sem = refs[:3], refs[3:6], refs[6]
    copies = [
        pltpu.make_async_copy(source, target, sem.at[n])
        for n, (source, target) in enumerate(zip(sources, targets))
    ]
    for copy in copies:
        copy.start()
    for copy in copies:
        copy.wait()


def body(sizes, bits, th, sh, pj, tq, tk, sq, sk, lengths, plan):
    ny, nz, nx = sizes
    rows = th.shape[0]
    d_s = sh.shape[1]
    half_t, half_s = tq.shape[1], sq.shape[1]
    bf16, f32 = jnp.bfloat16, jnp.float32
    table = lengths.reshape(-1, 128)
    any_spec = pl.BlockSpec(memory_space=pl.ANY)
    vmem_spec = pl.BlockSpec(memory_space=pltpu.VMEM)
    dma = pltpu.SemaphoreType.DMA
    plane = nz * nx
    scratch = [
        pltpu.VMEM((SLOTS, MAXLEN, half_t), bf16),
        pltpu.VMEM((SLOTS, MAXLEN, half_t), bf16),
        pltpu.VMEM((SLOTS, half_s, MAXLEN), bf16),
        pltpu.VMEM((SLOTS, half_s, MAXLEN), bf16),
        pltpu.VMEM((2 * SLOTS, HALF, half_t), bf16),
        pltpu.VMEM((2 * SLOTS, d_s, HALF), bf16),
        pltpu.VMEM((d_s, half_t), bf16),
        pltpu.VMEM(table.shape, jnp.int32),
        pltpu.SMEM(table.shape, jnp.int32),
        pltpu.SMEM(plan.shape, jnp.int32),
        pltpu.VMEM((SLOTS, MAXLEN, HALF), f32),
        pltpu.VMEM((SLOTS, MAXLEN, HALF), f32),
        pltpu.VMEM((SLOTS, MAXLEN, HALF), f32),
        pltpu.VMEM((SLOTS, 1, HALF), f32),
        pltpu.VMEM((SLOTS, 1, HALF), f32),
        pltpu.VMEM((2 * (plane - 1), 1, HALF), f32),
        pltpu.VMEM((4 * (ny - 1), 1, HALF), f32),
        pltpu.VMEM((2 * (2 * plane + SLOTS + 1), 1, HALF), f32),
        pltpu.VMEM((2 * ny + SLOTS + 1, 1, HALF), f32),
        pltpu.VMEM((SLOTS + 1, 1, HALF), f32),
        pltpu.VMEM((SLOTS + 1, 1, HALF), f32),
        pltpu.VMEM((SLOTS, 1, HALF), f32),
        dma((6 * SLOTS + 1 + 4 * SLOTS,)),
        dma((3,)),
        dma((SLOTS,)),
        dma((SLOTS,)),
        dma((2,)),
        dma((plane - 1,)),
        dma((2 * (plane - 1),)),
        dma((2 * (ny - 1),)),
        dma((ny - 1,)),
        dma((4,)),
        pltpu.SemaphoreType.REGULAR((2,)),
    ]
    shapes = ((2 * SLOTS, 128), (SLOTS, 1, HALF), (1, 128))
    results = pl.pallas_call(
        functools.partial(kernel, sizes, bits),
        name="distill",
        out_shape=tuple(pltpu.VMEM(shape, f32) for shape in shapes),
        in_specs=[any_spec] * 9,
        out_specs=(vmem_spec,) * 3,
        scratch_shapes=scratch,
        compiler_params=pltpu.CompilerParams(
            collective_id=0, has_side_effects=True, vmem_limit_bytes=60 * 1024 * 1024
        ),
        cost_estimate=pl.CostEstimate(
            flops=3_500_000_000, bytes_accessed=12_000_000, transcendentals=0
        ),
    )(th, sh.T, pj, tq, tk, sq.T, sk.T, table, plan)
    hid, row, loss = pl.pallas_call(
        deliver,
        name="deliver",
        out_shape=tuple(jax.ShapeDtypeStruct(shape, f32) for shape in shapes),
        in_specs=[vmem_spec] * 3,
        out_specs=(any_spec,) * 3,
        scratch_shapes=[dma((3,))],
    )(*(pltpu.with_memory_space_constraint(result, pltpu.VMEM) for result in results))
    return (
        hid.reshape(rows // 2),
        row.reshape(1, 1, SLOTS, HALF),
        loss[0, 0],
    )


def bit_groups(sizes):
    ny, nz, nx = sizes
    first = (nx * nz).bit_length() - 1
    return tuple(range(first)), tuple(range(first, first + ny.bit_length() - 1))


def solution(mesh, sizes=(4, 8, 4)):
    torus = Mesh(mesh.devices.reshape(*sizes, mesh.shape["head"]), DP_HEAD)
    placed = (
        P(DP, "head"),
        P(DP, None),
        P(None, "head"),
        P(DP, "head"),
        P(DP, "head"),
        P(DP, "head"),
        P(DP, "head"),
        P(),
        P(),
    )
    return jax.shard_map(
        functools.partial(body, sizes, bit_groups(sizes)),
        mesh=torus,
        in_specs=placed,
        out_specs=(P(DP_HEAD), P(DP, "head", None, None), P()),
        check_vma=False,
    )
```
